256 devices in a mesh: band: 64 (over x, z, core), dir: 4 (over y).
Axes of the slice: x: 4, y: 4, z: 8, core: 2. Of those that a mesh axis runs over, the one named last changes fastest.
Arguments:
- visibilities: bfloat16 [128, 32, 2, 256, 256], P('band', 'dir'), as said below
- sky_model: bfloat16 [128, 32, 2, 256, 256], P('band', 'dir')
- rfi_flags: int32 [128, 8, 8], P('band'), may hold values from 0 to 1, as said below
- destination: int32 [128], P('band'), may hold values from 0 to 127, as said below
Outputs:
- delivered: float32 [128, 32, 2, 256], P('band', 'dir')
- coefficients: float32 [9, 32, 2, 256], P(None, 'dir')
- norm_values: float32 [2, 2], replicated
The draws below stay inside these ranges and needn't reach their ends.
Inputs may be any that keep to these rules, and one draw needn't show every extreme that they name: `rfi_flags`: 1 marks a flagged baseline block; the share of flagged blocks tends to fall with the subband index. destination holds every row of 0 to 127 once. With the rows split into 64 aligned blocks of 2 rows, one row of block i goes to a row of block i + 1 and the other to a row of block i + 32, modulo 128 // 2. `visibilities`: visibilities follow the model under unknown station gains, with noise.
All inputs are finite; a program needn't handle non-finite values.
Results may differ from the reference program's by a relative error of at most 0.0003.
Values sent between devices are 32-bit elements; how exact they have to be, the bound alone decides.
A program may use at most 128 MiB of HBM per device.

```python
import jax
import jax.numpy as jnp
from jax import lax

STATIONS = 256
DIRECTIONS = 32
BLOCK = 32
DEGREE = 8
SWEEPS = 4
ITERS = 2
SB_DEV = 2
SUBBANDS = 128


def band_pair(key, band_row):
    band_key = jax.random.fold_in(jax.random.fold_in(key, 11), band_row)
    model_key, noise_key, rough_key = jax.random.split(band_key, 3)
    shared = jax.random.normal(jax.random.fold_in(key, 23), (4, DIRECTIONS, STATIONS), jnp.float32)
    rough = jax.random.normal(rough_key, (2, DIRECTIONS, STATIONS), jnp.float32)
    abscissa = (2.0 * band_row.astype(jnp.float32) + 1.0) / SUBBANDS - 1.0
    sky_values = jax.random.normal(model_key, (DIRECTIONS, 2, STATIONS, STATIONS), jnp.float32)
    noise_level = 0.5
    amp_spread = 0.25
    amplitude = 1.0 + amp_spread * shared[0] + 0.15 * abscissa * shared[1] + 0.1 * rough[0]
    phase = 0.8 * shared[2] + 0.5 * abscissa * shared[3] + 0.2 * rough[1]
    gain_re = amplitude * jnp.cos(phase)
    gain_im = amplitude * jnp.sin(phase)
    model_re = sky_values[:, 0]
    model_im = sky_values[:, 1]
    twist_re = model_re * gain_re[:, None, :] + model_im * gain_im[:, None, :]
    twist_im = model_im * gain_re[:, None, :] - model_re * gain_im[:, None, :]
    noise = jax.random.normal(noise_key, (2, DIRECTIONS, STATIONS, STATIONS), jnp.float32)
    data_re = gain_re[:, :, None] * twist_re - gain_im[:, :, None] * twist_im + noise_level * noise[0]
    data_im = gain_re[:, :, None] * twist_im + gain_im[:, :, None] * twist_re + noise_level * noise[1]
    return (sky_values.astype(jnp.bfloat16), jnp.stack([data_re, data_im], axis=1).astype(jnp.bfloat16))


def draw_sky_model(key, part):

    def one_band(band_row):
        return band_pair(key, band_row)[0]
    return lax.map(one_band, jnp.arange(SUBBANDS))


def draw_visibilities(key, part):

    def one_band(band_row):
        return band_pair(key, band_row)[1]
    return lax.map(one_band, jnp.arange(SUBBANDS))


def draw_rfi_flags(key, part):
    band_rows = jnp.arange(SUBBANDS)
    threshold = 750 - 600 * band_rows // max(SUBBANDS - 1, 1)
    blocks = STATIONS // BLOCK
    random_ints = jax.random.randint(jax.random.fold_in(key, 5), (SUBBANDS, blocks, blocks), 0, 1000)
    return (random_ints < threshold[:, None, None]).astype(jnp.int32)


def draw_destination(key, part):
    block_count = SUBBANDS // SB_DEV
    half_count = block_count // 2
    base_key = jax.random.fold_in(key, 7)
    send_key, recv_key = jax.random.split(base_key)
    send_perm = jax.vmap(lambda one_key: jax.random.permutation(one_key, SB_DEV))(jax.random.split(send_key, block_count))
    recv_perm = jax.vmap(lambda one_key: jax.random.permutation(one_key, SB_DEV))(jax.random.split(recv_key, block_count))
    block_ids = jnp.arange(block_count)[:, None]
    slot_ids = jnp.arange(SB_DEV)[None, :]
    source_rows = block_ids * SB_DEV + send_perm
    target_block = jnp.where(slot_ids == 0, (block_ids + 1) % block_count, jnp.where(slot_ids == 1, (block_ids + half_count) % block_count, block_ids + 0 * slot_ids))
    target_slot = recv_perm[target_block, slot_ids + 0 * block_ids]
    target_rows = target_block * SB_DEV + target_slot
    result = jnp.zeros((SUBBANDS,), jnp.int32).at[source_rows.reshape(-1)].set(target_rows.reshape(-1).astype(jnp.int32))
    return result.astype(jnp.int32)


def setup_inputs(seed: int = 0) -> dict:
    streams_of = jax.random.split(jax.random.key(seed), 5)
    return {
        "visibilities": draw_visibilities(jax.random.fold_in(streams_of[4], 71), 0),
        "sky_model": draw_sky_model(jax.random.fold_in(streams_of[4], 71), 0),
        "rfi_flags": draw_rfi_flags(jax.random.fold_in(streams_of[4], 71), 0),
        "destination": draw_destination(jax.random.fold_in(streams_of[4], 71), 0),
    }


highest = lax.Precision.HIGHEST
penalty_share = 0.4

def block_weights(rfi_flags):
    blocks = rfi_flags.shape[-1]
    kept_blocks = (1 - rfi_flags).astype(jnp.float32)
    leading = kept_blocks.shape[:-2]
    spread = jnp.broadcast_to(kept_blocks[..., :, None, :, None], leading + (blocks, BLOCK, blocks, BLOCK))
    stations = blocks * BLOCK
    spread = spread.reshape(leading + (stations, stations))
    return spread * (1.0 - jnp.eye(stations, dtype=jnp.float32))

def operators(visibilities, sky_model, rfi_flags):
    baseline = block_weights(rfi_flags)[..., None, :, :]
    data_re = visibilities[..., 0, :, :].astype(jnp.float32)
    data_im = visibilities[..., 1, :, :].astype(jnp.float32)
    model_re = sky_model[..., 0, :, :].astype(jnp.float32)
    model_im = sky_model[..., 1, :, :].astype(jnp.float32)
    oper_re = baseline * (model_re * data_re + model_im * data_im)
    oper_im = baseline * (model_re * data_im - model_im * data_re)
    square = baseline * (model_re * model_re + model_im * model_im)
    return (jnp.stack([oper_re, oper_im], axis=-3), square)

def chebyshev(band_rows, band_total):
    abscissa = (2.0 * band_rows + 1.0) / band_total - 1.0
    cheb_terms = [jnp.ones_like(abscissa), abscissa]
    for degree in range(2, DEGREE + 1):
        cheb_terms.append(2.0 * abscissa * cheb_terms[-1] - cheb_terms[-2])
    return jnp.stack(cheb_terms[:DEGREE + 1], axis=0)

def stefcal(operator, square, gain_now, target, penalty):
    pen_term = penalty[..., None, None, None]
    for sweep_index in range(SWEEPS):
        products = jnp.einsum('...kapq,...kbq->...kabp', operator, gain_now, precision=highest)
        real_part = products[..., 0, 0, :] - products[..., 1, 1, :]
        imag_part = products[..., 0, 1, :] + products[..., 1, 0, :]
        numerator = jnp.stack([real_part, imag_part], axis=-2)
        magnitude = lax.optimization_barrier(jnp.sum(gain_now * gain_now, axis=-2))
        denominator = jnp.einsum('...kpq,...kq->...kp', square, magnitude, precision=highest)
        updated = (numerator + pen_term * target) / (denominator[..., None, :] + pen_term)
        gain_now = 0.5 * (updated + gain_now) if sweep_index % 2 == 1 else updated
    return gain_now

def per_band(band_items):
    vis_band, model_band, flag_band, gain_band, target_band, pen_band = band_items
    operator, square = operators(vis_band, model_band, flag_band)
    return stefcal(operator, square, gain_band, target_band, pen_band)

def reference(visibilities, sky_model, rfi_flags, destination):
    band_total = visibilities.shape[0]
    directions = visibilities.shape[1]
    stations = visibilities.shape[-1]
    blocks = rfi_flags.shape[-1]
    weights = (1.0 + lax.optimization_barrier(jnp.sum(1 - rfi_flags, axis=(1, 2))).astype(jnp.float32)) / (1.0 + blocks * blocks)
    penalty = penalty_share * stations * weights
    cheb_basis = chebyshev(jnp.arange(band_total).astype(jnp.float32), band_total)
    weighted = cheb_basis * weights[None, :]
    gram_matrix = jnp.dot(weighted, cheb_basis.T, precision=highest)
    factor = jnp.linalg.cholesky(gram_matrix)
    normalizer = directions * 2.0 * stations * gram_matrix[0, 0]
    ones_part = jnp.ones((band_total, directions, stations), jnp.float32)
    unit_gains = jnp.stack([ones_part, jnp.zeros_like(ones_part)], axis=2)
    gain_now = unit_gains
    consensus = unit_gains
    dual_var = jnp.zeros_like(unit_gains)
    row_weight = weights[:, None, None, None]
    norm_rows = []
    coefficients = None
    for iteration in range(ITERS):
        gain_now = lax.map(per_band, (visibilities, sky_model, rfi_flags, gain_now, consensus - dual_var, penalty))
        projection = jnp.einsum('cs,skap->ckap', weighted, gain_now + dual_var, precision=highest)
        flat_proj = projection.reshape(projection.shape[0], -1)
        coefficients = jax.scipy.linalg.cho_solve((factor, True), flat_proj).reshape(projection.shape)
        fresh_gains = jnp.einsum('cs,ckap->skap', cheb_basis, coefficients, precision=highest)
        dual_var = dual_var + gain_now - fresh_gains
        primal = jnp.sqrt(jnp.sum(row_weight * (gain_now - fresh_gains) ** 2) / normalizer)
        dual_norm = jnp.sqrt(jnp.sum(row_weight * (fresh_gains - consensus) ** 2) / normalizer)
        norm_rows.append(jnp.stack([primal, dual_norm]))
        consensus = fresh_gains
    delivered = jnp.zeros_like(gain_now).at[destination].set(gain_now)
    return (delivered, coefficients, jnp.stack(norm_rows))
```

```python
import jax
import jax.numpy as jnp
from jax import lax
from jax.experimental import pallas as pl
from jax.experimental.pallas import tpu as pltpu
from jax.sharding import PartitionSpec as P

DEGREE = 8
SWEEPS = 4
TERMS = DEGREE + 1
BANDS = 64
OWNERS = 32
DIRS = 4
ROWS = 16
HALF = 128

f32 = jnp.float32
bf16 = jnp.bfloat16
HIGHEST = lax.Precision.HIGHEST
MESH = pl.DeviceIdType.MESH
penalty_share = 0.4


def iota(shape, dim):
    return lax.broadcasted_iota(jnp.int32, shape, dim)


def gather(x, index, axis):
    return jnp.take_along_axis(x, index, axis=axis, mode="promise_in_bounds")


def dot(a, b, contract):
    return lax.dot_general(
        a, b, (contract, ((), ())), precision=HIGHEST, preferred_element_type=f32
    )


def kernel(
    flags, dest, vis, sky, dlv_out, coef_out, norm_out,
    visb, skyb, are, aim, bsq, tre, tim, tmag, num, row, tgt, pens,
    wsend, wrecv, asend, arecv, bsend, brecv, csend, crecv, near_s, far_s, near_r, far_r,
    dsend, drecv, esend, erecv, proj, spread, norm0, dummy,
    in_sem, w_ss, w_rs, a_ss, a_rs, b_ss, b_rs, c_ss, c_rs, n_ss, n_rs, f_ss, f_rs,
    d_ss, d_rs, e_ss, e_rs,
):
    me = lax.axis_index("band")
    plane = lax.axis_index("dir")
    chip = me // 2
    core = lax.rem(me, 2)

    def copy_to(src, dst, ss, rs, target):
        return pltpu.make_async_remote_copy(
            src_ref=src, dst_ref=dst, send_sem=ss, recv_sem=rs,
            device_id={"band": target}, device_id_type=MESH,
        )

    def chunk(i, arr, buf, s):
        f, c = i // 4, lax.rem(i, 4)
        rows = pl.ds(pl.multiple_of(c * 64, 64), 64)
        return pltpu.make_async_copy(
            arr.at[f, :, :, rows, :], buf.at[f, :, :, rows, :], in_sem.at[s, i]
        )

    for i in range(8):
        chunk(i, vis, visb, 0).start()
        chunk(i, sky, skyb, 1).start()

    barrier = pltpu.get_barrier_semaphore()

    def greet(t, _):
        pl.semaphore_signal(
            barrier, inc=1, device_id={"band": lax.rem(me + t, BANDS)}, device_id_type=MESH
        )
        return 0

    lax.fori_loop(1, BANDS, greet, 0)
    for t in range(1, DIRS):
        pl.semaphore_signal(
            barrier, inc=1, device_id={"dir": lax.rem(plane + t, DIRS)}, device_id_type=MESH
        )

    for f in range(2):
        count = jnp.int32(0)
        for a in range(8):
            for b in range(8):
                count = count + (1 - flags[f, a, b])
        weight = (1.0 + jnp.full((8, HALF), count, jnp.int32).astype(f32)) / 65.0
        pens[f] = penalty_share * 256.0 * weight
        wsend[pl.ds(f, 1), :] = weight[0:1, :]

    lane16 = lax.rem(iota((8, HALF), 1), 16)
    group = iota((8, HALF), 1) // 16
    sub = iota((8, HALF), 0)
    spread_index = [group * 16 + half * 8 + sub for half in range(2)]
    mix1 = lax.rem(group + sub, 8) * 16 + lane16
    mix2 = lax.rem(sub - group + 8, 8)
    mix3 = lax.rem(sub - group + 8, 8) * 16 + lane16

    def swap_groups(x):
        return gather(gather(gather(x, mix1, 1), mix2, 0), mix3, 1)

    q_lane = iota((ROWS, HALF), 1)
    p_sub = iota((ROWS, HALF), 0)

    def operator_block(t, _):
        f, ph = t // ROWS, lax.rem(t, ROWS)

        @pl.when(lax.rem(ph, 4) == 0)
        def _():
            i = t // 4
            chunk(i, vis, visb, 0).wait()
            chunk(i, sky, skyb, 1).wait()

        rows = pl.ds(pl.multiple_of(ph * ROWS, ROWS), ROWS)
        sums = []
        for qh in range(2):
            keep = [
                jnp.full((ROWS, HALF), 1 - flags[f, ph // 2, qh * 4 + b], jnp.int32)
                for b in range(4)
            ]
            kept = keep[3]
            for b in (2, 1, 0):
                kept = jnp.where(q_lane < (b + 1) * 32, keep[b], kept)
            apart = q_lane + qh * HALF != p_sub + ph * ROWS
            mask = jnp.where(apart, kept, 0).astype(f32).astype(bf16)[None]
            lanes = pl.ds(qh * HALF, HALF)

            def flipped(x):
                return x.reshape(HALF, HALF).T.astype(f32)

            mr = flipped(skyb[f, :, 0, rows, lanes] * mask)
            mi = flipped(skyb[f, :, 1, rows, lanes] * mask)
            dr = flipped(visb[f, :, 0, rows, lanes])
            di = flipped(visb[f, :, 1, rows, lanes])
            ar = mr * dr + mi * di
            ai = mr * di - mi * dr
            b2 = mr * mr + mi * mi
            are[f, ph, pl.ds(qh * HALF, HALF), :] = ar
            aim[f, ph, pl.ds(qh * HALF, HALF), :] = ai
            bsq[f, ph, pl.ds(qh * HALF, HALF), :] = b2
            sums.append([jnp.sum(v, axis=0, keepdims=True) for v in (ar, ai, b2)])
        for n in range(3):
            num[f, n, pl.ds(ph, 1), :] = sums[0][n] + sums[1][n]
        return 0

    lax.fori_loop(0, 2 * ROWS, operator_block, 0)

    pl.semaphore_wait(barrier, BANDS - 1 + DIRS - 1)

    def to_owners(src_of, dst, ss, rs):
        def send(t, _):
            j = lax.rem(chip + t, OWNERS)
            copy_to(src_of(j), dst.at[me], ss, rs, 2 * j + 1).start()
            return 0

        lax.fori_loop(1, OWNERS, send, 0)

        @pl.when(core == 0)
        def _():
            copy_to(src_of(chip), dst.at[me], ss, rs, me + 1).start()

    to_owners(lambda j: wsend, wrecv, w_ss, w_rs)

    @pl.when(core == 1)
    def _():
        wrecv[me] = wsend[...]

    ones = jnp.ones((ROWS, HALF), f32)
    zeros = jnp.zeros((ROWS, HALF), f32)
    for f in range(2):
        row[f, 0] = ones
        row[f, 1] = zeros
        tgt[f, 0] = ones
        tgt[f, 1] = zeros

    def update(f, odd):
        pen = jnp.concatenate([pens[f], pens[f]], axis=0)
        below = num[f, 2] + pen
        new = []
        for part in range(2):
            fresh = (num[f, part] + pen * tgt[f, part]) / below
            fresh = jnp.where(odd, 0.5 * (fresh + row[f, part]), fresh)
            row[f, part] = fresh
            new.append(fresh)
        return new

    def tiles(f, new):
        for ph in range(ROWS):
            for half in range(2):
                at = pl.ds(ph * ROWS + half * 8, 8)
                t = [
                    gather(
                        jnp.broadcast_to(v[ph : ph + 1, :], (8, HALF)), spread_index[half], 1
                    )
                    for v in new
                ]
                tre[f, at, :] = t[0]
                tim[f, at, :] = t[1]
                tmag[f, at, :] = t[0] * t[0] + t[1] * t[1]

    GROUP = 4

    def matvec(f):
        def block(pb, _):
            acc = [[jnp.zeros((8, HALF), f32) for _ in range(3)] for _ in range(GROUP)]
            for q in range(32):
                at = pl.ds(q * 8, 8)
                gr, gi, gm = tre[f, at, :], tim[f, at, :], tmag[f, at, :]
                for j in range(GROUP):
                    ph = pb * GROUP + j
                    a, b = are[f, ph, at, :], aim[f, ph, at, :]
                    acc[j][0] = acc[j][0] + (a * gr - b * gi)
                    acc[j][1] = acc[j][1] + (a * gi + b * gr)
                    acc[j][2] = acc[j][2] + bsq[f, ph, at, :] * gm
            for j in range(GROUP):
                for n in range(3):
                    num[f, n, pl.ds(pb * GROUP + j, 1), :] = jnp.sum(
                        acc[j][n], axis=0, keepdims=True
                    )
            return 0

        lax.fori_loop(0, ROWS // GROUP, block, 0)

    def sweep(s, f):
        matvec(f)
        tiles(f, update(f, lax.rem(s, 2) == 1))
        return 0

    for f in range(2):
        tiles(f, update(f, False))

    def sweeps(t, _):
        return sweep(t // 2, lax.rem(t, 2))

    lax.fori_loop(2, 2 * SWEEPS, sweeps, 0)

    def natural(f):
        return [
            [swap_groups(row[f, part, h * 8 : h * 8 + 8, :]) for h in range(2)]
            for part in range(2)
        ]

    def pack(dst):
        for f in range(2):
            n = natural(f)
            for part in range(2):
                for h in range(2):
                    dst[pl.ds((part * 2 + h) * 8, 8), f, :] = n[part][h]

    pack(asend)
    to_owners(lambda j: asend.at[j], arecv, a_ss, a_rs)

    def both(ref):
        return jnp.concatenate([ref[:, 0, :], ref[:, 1, :]], axis=0)

    def await_bytes(ref, ss, rs, sent):
        c = copy_to(ref, ref, ss, rs, lax.rem(me + 1, BANDS))
        c.wait_send() if sent else c.wait_recv()

    @pl.when(core == 1)
    def _():
        arecv[me] = asend[chip]
        await_bytes(wrecv.at[pl.ds(0, BANDS - 1)], w_ss, w_rs, False)
        weight = both(wrecv)
        r = iota((HALF, HALF), 0)
        lane = iota((HALF, HALF), 1)
        band_row = (lax.rem(r, BANDS) * 2 + r // BANDS).astype(f32)
        x = (2.0 * band_row + 1.0) / 128.0 - 1.0
        basis = jnp.where(lane == 0, 1.0, jnp.where(lane == 1, x, 0.0))
        before, now = jnp.ones_like(x), x
        for c in range(2, TERMS):
            before, now = now, 2.0 * x * now - before
            basis = jnp.where(lane == c, now, basis)
        weighted = basis * weight
        gram = dot(weighted, basis, ((0,), (0,)))[:ROWS, :]
        r16, l16 = iota((ROWS, HALF), 0), iota((ROWS, HALF), 1)
        m = jnp.where((r16 >= TERMS) & (l16 == r16), 1.0, gram)
        m = jnp.where(l16 == r16 + 16, 1.0, m)
        for c in range(TERMS):
            line = m[c : c + 1, :] / m[c : c + 1, c : c + 1]
            m = jnp.where(r16 == c, line, m - m[:, c : c + 1] * line)
        inverse = m[:, 16:32]
        proj[...] = dot(inverse, weighted[:, :ROWS], ((1,), (1,)))
        spread[...] = dot(basis[:, :ROWS], proj[...], ((1,), (0,)))
        scale = 1.0 / (16384.0 * jnp.sum(weight, axis=0, keepdims=True))

        await_bytes(arecv.at[pl.ds(0, BANDS - 1)], a_ss, a_rs, False)
        gain = both(arecv)
        fresh = dot(spread[...], gain, ((1,), (0,)))
        bsend[:, 0, :] = fresh[:BANDS, :]
        bsend[:, 1, :] = fresh[BANDS:, :]

        def back(t, _):
            i = lax.rem(me + t, BANDS)
            copy_to(bsend.at[i], brecv.at[chip], b_ss, b_rs, i).start()
            return 0

        lax.fori_loop(1, BANDS, back, 0)
        brecv[chip] = bsend[me]
        first = jnp.where(chip < 16, 1.0, 0.0)
        norm0[0:1, :] = scale * jnp.sum(weight * (gain - fresh) ** 2, axis=0, keepdims=True)
        norm0[1:2, :] = scale * jnp.sum(weight * (fresh - first) ** 2, axis=0, keepdims=True)
        norm0[2:3, :] = scale
        await_bytes(brecv.at[pl.ds(0, OWNERS - 1)], b_ss, b_rs, False)

    @pl.when(core == 0)
    def _():
        await_bytes(brecv, b_ss, b_rs, False)

    for f in range(2):
        for part in range(2):
            for h in range(2):
                lines = brecv[pl.ds((part * 2 + h) * 8, 8), f, :]
                at = slice(h * 8, h * 8 + 8)
                tgt[f, part, at, :] = 2.0 * swap_groups(lines) - row[f, part, at, :]

    lax.fori_loop(0, 2 * SWEEPS, sweeps, 0)

    pack(csend)
    to_owners(lambda j: csend.at[j], crecv, c_ss, c_rs)

    near = lax.rem(me + 1, BANDS)
    far = lax.rem(me + BANDS // 2, BANDS)
    first_near = jnp.full((OWNERS, HALF), dest[0] // 2, jnp.int32) == near
    row_a, row_b = csend[:, 0, :], csend[:, 1, :]
    near_rows = jnp.where(first_near, row_a, row_b)
    far_rows = jnp.where(first_near, row_b, row_a)
    near_s[pl.ds(0, OWNERS), 0, :] = near_rows
    far_s[...] = far_rows.reshape(OWNERS, 1, HALF)
    slots = [jnp.full((1, HALF), lax.rem(dest[f], 2), jnp.int32).astype(f32) for f in range(2)]
    near_s[pl.ds(OWNERS, 1), 0, :] = jnp.where(first_near[:1], slots[0], slots[1])
    copy_to(near_s, near_r, n_ss, n_rs, near).start()
    copy_to(far_s, far_r, f_ss, f_rs, far).start()

    @pl.when(core == 1)
    def _():
        crecv[me] = csend[chip]
        gain0 = both(arecv)
        fresh0 = both(bsend)
        weight = both(wrecv)
        scale = norm0[2:3, :]
        await_bytes(crecv.at[pl.ds(0, BANDS - 1)], c_ss, c_rs, False)
        gain = both(crecv)
        moved = gain + (gain0 - fresh0)
        coef = dot(proj[...], moved, ((1,), (0,)))
        fresh = dot(spread[...], moved, ((1,), (0,)))
        primal = scale * jnp.sum(weight * (gain - fresh) ** 2, axis=0, keepdims=True)
        dual = scale * jnp.sum(weight * (fresh - fresh0) ** 2, axis=0, keepdims=True)
        lane = iota((1, HALF), 1)
        line = jnp.zeros((1, HALF), f32)
        for n, v in enumerate((norm0[0:1, :], norm0[1:2, :], primal, dual)):
            line = jnp.where(lane == n, jnp.sum(v, axis=1, keepdims=True), line)
        for k in range(5):
            dsend[k] = coef[2 * k : 2 * k + 2, :]
        dsend[4, pl.ds(1, 1), :] = line

        def spread_out(t, _):
            i = lax.rem(me + t, BANDS)
            copy_to(dsend, drecv.at[chip], d_ss, d_rs, i).start()
            return 0

        lax.fori_loop(1, BANDS, spread_out, 0)
        drecv[chip] = dsend[...]

    await_bytes(near_r, n_ss, n_rs, False)
    await_bytes(far_r, f_ss, f_rs, False)
    slot = near_r[OWNERS, 0:1, :]
    for part in range(2):
        for h in range(2):
            at = pl.ds((part * 2 + h) * 8, 8)
            a, b = near_r[at, 0, :], far_r[at, 0, :]
            swap = jnp.broadcast_to(slot, (8, HALF)) > 0.5
            lanes = pl.ds(h * HALF, HALF)
            dlv_out[0, :, part, lanes] = jnp.where(swap, b, a)
            dlv_out[1, :, part, lanes] = jnp.where(swap, a, b)

    @pl.when(core == 1)
    def _():
        await_bytes(drecv.at[pl.ds(0, OWNERS - 1)], d_ss, d_rs, False)

    @pl.when(core == 0)
    def _():
        await_bytes(drecv, d_ss, d_rs, False)

    esend[...] = jnp.sum(drecv[:, 4, 1, :], axis=0, keepdims=True)
    for t in range(1, DIRS):
        pltpu.make_async_remote_copy(
            src_ref=esend, dst_ref=erecv.at[t - 1], send_sem=e_ss, recv_sem=e_rs.at[t - 1],
            device_id={"dir": lax.rem(plane + t, DIRS)}, device_id_type=MESH,
        ).start()
    for c in range(TERMS):
        for part in range(2):
            for h in range(2):
                at = pl.ds((part * 2 + h) * 8, 8)
                coef_out[c, :, part, pl.ds(h * HALF, HALF)] = drecv[at, c // 2, c % 2, :]
    total = esend[...]
    for t in range(1, DIRS):
        pltpu.make_async_remote_copy(
            src_ref=esend, dst_ref=erecv.at[t - 1], send_sem=e_ss, recv_sem=e_rs.at[t - 1],
            device_id={"dir": lax.rem(plane + t, DIRS)}, device_id_type=MESH,
        ).wait_recv()
    for t in range(1, DIRS):
        total = total + erecv[t - 1]
    norm_out[...] = jnp.sqrt(total)

    await_bytes(erecv, e_ss, e_rs.at[0], True)
    await_bytes(near_s, n_ss, n_rs, True)
    await_bytes(far_s, f_ss, f_rs, True)

    @pl.when(core == 1)
    def _():
        await_bytes(wrecv.at[pl.ds(0, OWNERS - 1)], w_ss, w_rs, True)
        await_bytes(asend.at[pl.ds(0, OWNERS - 1)], a_ss, a_rs, True)
        await_bytes(csend.at[pl.ds(0, OWNERS - 1)], c_ss, c_rs, True)
        await_bytes(bsend.at[pl.ds(0, BANDS - 1)], b_ss, b_rs, True)
        await_bytes(dummy, d_ss, d_rs, True)

    @pl.when(core == 0)
    def _():
        await_bytes(wrecv.at[pl.ds(0, OWNERS)], w_ss, w_rs, True)
        await_bytes(asend, a_ss, a_rs, True)
        await_bytes(csend, c_ss, c_rs, True)


def per_device(visibilities, sky_model, rfi_flags, destination):
    vmem = pltpu.VMEM
    dma = pltpu.SemaphoreType.DMA
    big = vmem((2, ROWS, 256, HALF), f32)
    tile = vmem((2, 256, HALF), f32)
    lines = vmem((OWNERS, 2, HALF), f32)
    every = vmem((BANDS, 2, HALF), f32)
    scratch = [
        vmem((2, 8, 2, 256, 256), bf16), vmem((2, 8, 2, 256, 256), bf16),
        big, big, big, tile, tile, tile,
        vmem((2, 3, ROWS, HALF), f32), vmem((2, 2, ROWS, HALF), f32),
        vmem((2, 2, ROWS, HALF), f32), vmem((2, 8, HALF), f32),
        vmem((2, HALF), f32), every, lines, every, every, lines, lines, every,
        vmem((OWNERS + 1, 1, HALF), f32), vmem((OWNERS, 1, HALF), f32),
        vmem((OWNERS + 1, 1, HALF), f32), vmem((OWNERS, 1, HALF), f32),
        vmem((5, 2, HALF), f32), vmem((OWNERS, 5, 2, HALF), f32),
        vmem((1, HALF), f32), vmem((DIRS - 1, 1, HALF), f32),
        vmem((ROWS, HALF), f32), vmem((HALF, HALF), f32), vmem((8, HALF), f32),
        vmem((BANDS - 1, 5, 2, HALF), f32),
        dma((2, 8)), *([dma(())] * 15), dma((DIRS - 1,)),
    ]
    smem = pl.BlockSpec(memory_space=pltpu.SMEM)
    hbm = pl.BlockSpec(memory_space=pl.ANY)
    inside = pl.BlockSpec(memory_space=pltpu.VMEM)
    delivered, coefficients, norms = pl.pallas_call(
        kernel,
        out_shape=(
            jax.ShapeDtypeStruct((2, 8, 2, 256), f32),
            jax.ShapeDtypeStruct((TERMS, 8, 2, 256), f32),
            jax.ShapeDtypeStruct((1, HALF), f32),
        ),
        in_specs=[smem, smem, hbm, hbm],
        out_specs=(inside, inside, inside),
        scratch_shapes=scratch,
        compiler_params=pltpu.CompilerParams(
            collective_id=0, has_side_effects=True, vmem_limit_bytes=48 * 1024 * 1024
        ),
        name="admm",
    )(rfi_flags, destination, visibilities, sky_model)
    return delivered, coefficients, norms[0, :4].reshape(2, 2)


def solution(mesh):
    return jax.shard_map(
        per_device,
        mesh=mesh,
        in_specs=(
            P("band", "dir", None, None, None),
            P("band", "dir", None, None, None),
            P("band", None, None),
            P("band"),
        ),
        out_specs=(P("band", "dir", None, None), P(None, "dir", None, None), P()),
        check_vma=False,
    )
```

```python
import jax
import jax.numpy as jnp
from jax import lax
from jax.experimental import pallas as pl
from jax.experimental.pallas import tpu as pltpu
from jax.sharding import PartitionSpec as P

DEGREE = 8
SWEEPS = 4
TERMS = DEGREE + 1
BANDS = 64
OWNERS = 32
DIRS = 4
ROWS = 16
HALF = 128

f32 = jnp.float32
bf16 = jnp.bfloat16
HIGHEST = lax.Precision.HIGHEST
MESH = pl.DeviceIdType.MESH
penalty_share = 0.4


def iota(shape, dim):
    return lax.broadcasted_iota(jnp.int32, shape, dim)


def gather(x, index, axis):
    return jnp.take_along_axis(x, index, axis=axis, mode="promise_in_bounds")


def dot(a, b, contract):
    return lax.dot_general(
        a, b, (contract, ((), ())), precision=HIGHEST, preferred_element_type=f32
    )


def hops(t):
    x, z = t // 8, t % 8
    return min(x, 4 - x) + min(z, 8 - z)


FAR_FIRST = sorted(range(1, OWNERS), key=lambda t: -hops(t))


def kernel(
    flags_hbm, dest_hbm, vis, sky, dlv_out, coef_out, norm_out,
    flags, dest, visb, skyb, are, aim, bsq, tc, tm, tp, tmag, num, row, tgt, pens,
    wsend, wrecv, asend, arecv, bsend, brecv, csend, crecv, near_s, far_s, near_r, far_r,
    dsend, drecv, esend, erecv, nsend, nrecv, proj, spread, norm0, dummy,
    in_sem, s_sem, w_ss, w_rs, a_ss, a_rs, b_ss, b_rs, c_ss, c_rs, n_ss, n_rs, f_ss, f_rs,
    d_ss, d_rs, e_ss, m_ss, m_rs, e_rs,
):
    me = lax.axis_index("band")
    plane = lax.axis_index("dir")
    chip = me // 2
    core = me - 2 * chip

    def wrapped(i, count):
        return jnp.where(i >= count, i - count, i)

    def copy_to(src, dst, ss, rs, target):
        return pltpu.make_async_remote_copy(
            src_ref=src, dst_ref=dst, send_sem=ss, recv_sem=rs,
            device_id={"band": target}, device_id_type=MESH,
        )

    def chunk(i, arr, buf, s):
        f, c = i // 4, lax.rem(i, 4)
        rows = pl.ds(pl.multiple_of(c * 64, 64), 64)
        return pltpu.make_async_copy(
            arr.at[f, :, :, rows, :], buf.at[f, :, :, rows, :], in_sem.at[s, i]
        )

    for i in range(8):
        chunk(i, vis, visb, 0).start()
        chunk(i, sky, skyb, 1).start()

    small = [
        pltpu.make_async_copy(flags_hbm, flags, s_sem.at[0]),
        pltpu.make_async_copy(dest_hbm, dest, s_sem.at[1]),
    ]
    for c in small:
        c.start()

    barrier = pltpu.get_barrier_semaphore()
    far = wrapped(me + BANDS // 2, BANDS)

    def greet(where):
        pl.semaphore_signal(barrier, inc=1, device_id=where, device_id_type=MESH)

    for t in FAR_FIRST:
        greet({"band": 2 * wrapped(chip + t, OWNERS) + 1})

    @pl.when(core == 0)
    def _():
        greet({"band": me + 1})
        greet({"band": far})

    @pl.when(core == 1)
    def _():
        for t in FAR_FIRST:
            greet({"band": 2 * wrapped(chip + t, OWNERS)})
        greet({"band": me - 1})
        for t in range(1, DIRS):
            greet({"dir": wrapped(plane + t, DIRS)})

    for c in small:
        c.wait()
    for f in range(2):
        count = jnp.int32(0)
        for a in range(8):
            for b in range(8):
                count = count + (1 - flags[f, a, b])
        weight = (1.0 + jnp.full((8, HALF), count, jnp.int32).astype(f32)) / 65.0
        pens[f] = penalty_share * 256.0 * weight
        wsend[pl.ds(f, 1), :] = weight[0:1, :]

    lane16 = iota((8, HALF), 1) % 16
    group = iota((8, HALF), 1) // 16
    sub = iota((8, HALF), 0)
    spread_index = [group * 16 + half * 8 + sub for half in range(2)]
    mix1 = (group + sub) % 8 * 16 + lane16
    mix2 = (sub - group + 8) % 8
    mix3 = (sub - group + 8) % 8 * 16 + lane16

    def swap_groups(x):
        return gather(gather(gather(x, mix1, 1), mix2, 0), mix3, 1)

    q_lane = iota((ROWS, HALF), 1)
    p_sub = iota((ROWS, HALF), 0)

    def operator_block(t, _):
        f, block = t // 8, t % 8

        @pl.when(block % 2 == 0)
        def _():
            chunk(t // 2, vis, visb, 0).wait()
            chunk(t // 2, sky, skyb, 1).wait()

        for qh in range(2):
            keep = [
                jnp.full((ROWS, HALF), 1 - flags[f, block, qh * 4 + b], jnp.int32)
                for b in range(4)
            ]
            kept = keep[3]
            for b in (2, 1, 0):
                kept = jnp.where(q_lane < (b + 1) * 32, keep[b], kept)
            lanes = pl.ds(qh * HALF, HALF)
            for u in range(2):
                ph = block * 2 + u
                rows = pl.ds(pl.multiple_of(ph * ROWS, ROWS), ROWS)
                apart = q_lane + qh * HALF != p_sub + ph * ROWS
                mask = jnp.where(apart, kept, 0).astype(f32).astype(bf16)[None]

                def flipped(x):
                    return x.reshape(HALF, HALF).T.astype(f32)

                mr = flipped(skyb[f, :, 0, rows, lanes] * mask)
                mi = flipped(skyb[f, :, 1, rows, lanes] * mask)
                dr = flipped(visb[f, :, 0, rows, lanes])
                di = flipped(visb[f, :, 1, rows, lanes])
                ar = mr * dr + mi * di
                ai = mr * di - mi * dr
                b2 = mr * mr + mi * mi
                are[f, ph, lanes, :] = ar
                aim[f, ph, lanes, :] = ai
                bsq[f, ph, lanes, :] = b2
                for n, v in enumerate((ar, ai, b2)):
                    part = jnp.sum(v, axis=0, keepdims=True)
                    if qh == 0:
                        num[f, n, pl.ds(ph, 1), :] = part
                    else:
                        num[f, n, pl.ds(ph, 1), :] = num[f, n, pl.ds(ph, 1), :] + part
        return 0

    lax.fori_loop(0, ROWS, operator_block, 0)

    def to_owners(src_of, dst, ss, rs):
        for t in FAR_FIRST:
            j = wrapped(chip + t, OWNERS)
            copy_to(src_of(j), dst.at[me], ss, rs, 2 * j + 1).start()

        @pl.when(core == 0)
        def _():
            copy_to(src_of(chip), dst.at[me], ss, rs, me + 1).start()

    def to_plane(src_of, dst, ss, rs):
        for t in FAR_FIRST:
            i = 2 * wrapped(chip + t, OWNERS)
            for k in range(2):
                copy_to(src_of(i + k), dst.at[chip], ss, rs, i + k).start()
        copy_to(src_of(me - 1), dst.at[chip], ss, rs, me - 1).start()

    @pl.when(core == 1)
    def _():
        wrecv[me] = wsend[...]

    ones = jnp.ones((ROWS, HALF), f32)
    zeros = jnp.zeros((ROWS, HALF), f32)
    for f in range(2):
        row[f, 0] = ones
        row[f, 1] = zeros
        tgt[f, 0] = ones
        tgt[f, 1] = zeros

    def update(f, odd):
        pen = jnp.concatenate([pens[f], pens[f]], axis=0)
        below = num[f, 2] + pen
        for part in range(2):
            fresh = (num[f, part] + pen * tgt[f, part]) / below
            row[f, part] = jnp.where(odd, 0.5 * (fresh + row[f, part]), fresh)

    def tile_row(f, r):
        for half in range(2):
            at = pl.ds(pl.multiple_of(r * ROWS + half * 8, 8), 8)
            c, d = [
                gather(
                    jnp.broadcast_to(row[f, part, pl.ds(r, 1), :], (8, HALF)),
                    spread_index[half],
                    1,
                )
                for part in range(2)
            ]
            tc[f, at, :] = c
            tm[f, at, :] = d - c
            tp[f, at, :] = d + c
            tmag[f, at, :] = c * c + d * d

    GROUP = 8

    def sweep(f, odd):
        def block(pb, _):
            acc = [[jnp.zeros((8, HALF), f32) for _ in range(4)] for _ in range(GROUP)]
            for q in range(32):
                at = pl.ds(q * 8, 8)
                c, m, p, g = tc[f, at, :], tm[f, at, :], tp[f, at, :], tmag[f, at, :]
                for j in range(GROUP):
                    ph = pb * GROUP + j
                    a, b = are[f, ph, at, :], aim[f, ph, at, :]
                    terms = ((a + b) * c, a * m, b * p, bsq[f, ph, at, :] * g)
                    acc[j] = [x + y for x, y in zip(acc[j], terms)]
            for j in range(GROUP):
                k1, k2, k3, below = acc[j]
                for n, v in enumerate((k1 - k3, k1 + k2, below)):
                    num[f, n, pl.ds(pb * GROUP + j, 1), :] = jnp.sum(v, axis=0, keepdims=True)
            for j in range(GROUP):
                tile_row(1 - f, pb * GROUP + j)
            return 0

        lax.fori_loop(0, ROWS // GROUP, block, 0)
        update(f, odd)

    for f in range(2):
        update(f, False)
    lax.fori_loop(0, ROWS, lambda r, _: (tile_row(0, r), 0)[1], 0, unroll=True)

    def sweeps(t, _):
        sweep(t % 2, t // 2 % 2 == 1)
        return 0

    lax.fori_loop(2, 4, sweeps, 0)

    pl.semaphore_wait(barrier, jnp.where(core == 1, BANDS - 1 + DIRS - 1, OWNERS + 1))
    to_owners(lambda j: wsend, wrecv, w_ss, w_rs)

    lax.fori_loop(4, 2 * SWEEPS, sweeps, 0)

    def natural(f):
        return [
            [swap_groups(row[f, part, h * 8 : h * 8 + 8, :]) for h in range(2)]
            for part in range(2)
        ]

    def pack(dst):
        for f in range(2):
            n = natural(f)
            for part in range(2):
                for h in range(2):
                    dst[pl.ds((part * 2 + h) * 8, 8), f, :] = n[part][h]

    pack(asend)
    to_owners(lambda j: asend.at[j], arecv, a_ss, a_rs)

    def along(t):
        return pltpu.make_async_remote_copy(
            src_ref=esend, dst_ref=erecv.at[t - 1], send_sem=e_ss, recv_sem=e_rs.at[t - 1],
            device_id={"dir": wrapped(plane + t, DIRS)}, device_id_type=MESH,
        )

    def both(ref):
        return jnp.concatenate([ref[:, 0, :], ref[:, 1, :]], axis=0)

    near = wrapped(me + 1, BANDS)

    def await_bytes(ref, ss, rs, sent):
        c = copy_to(ref, ref, ss, rs, near)
        c.wait_send() if sent else c.wait_recv()

    @pl.when(core == 1)
    def _():
        arecv[me] = asend[chip]
        wrecv[me] = wsend[...]
        await_bytes(wrecv.at[pl.ds(0, BANDS - 1)], w_ss, w_rs, False)
        weight = both(wrecv)
        r = iota((HALF, HALF), 0)
        lane = iota((HALF, HALF), 1)
        band_row = (r % BANDS * 2 + r // BANDS).astype(f32)
        x = (2.0 * band_row + 1.0) / 128.0 - 1.0
        basis = jnp.where(lane == 0, 1.0, jnp.where(lane == 1, x, 0.0))
        before, now = jnp.ones_like(x), x
        for c in range(2, TERMS):
            before, now = now, 2.0 * x * now - before
            basis = jnp.where(lane == c, now, basis)
        weighted = basis * weight
        gram = dot(weighted, basis, ((0,), (0,)))[:ROWS, :]
        r16, l16 = iota((ROWS, HALF), 0), iota((ROWS, HALF), 1)
        m = jnp.where((r16 >= TERMS) & (l16 == r16), 1.0, gram)
        m = jnp.where(l16 == r16 + 16, 1.0, m)
        for c in range(TERMS):
            line = m[c : c + 1, :] / m[c : c + 1, c : c + 1]
            m = jnp.where(r16 == c, line, m - m[:, c : c + 1] * line)
        inverse = m[:, 16:32]
        proj[...] = dot(inverse, weighted[:, :ROWS], ((1,), (1,)))
        spread[...] = dot(basis[:, :ROWS], proj[...], ((1,), (0,)))
        scale = 1.0 / (16384.0 * jnp.sum(weight, axis=0, keepdims=True))

        await_bytes(arecv.at[pl.ds(0, BANDS - 1)], a_ss, a_rs, False)
        gain = both(arecv)
        fresh = dot(spread[...], gain, ((1,), (0,)))
        bsend[:, 0, :] = fresh[:BANDS, :]
        bsend[:, 1, :] = fresh[BANDS:, :]

        to_plane(lambda i: bsend.at[i], brecv, b_ss, b_rs)
        brecv[chip] = bsend[me]
        first = jnp.where(chip < 16, 1.0, 0.0)
        norm0[0:1, :] = scale * jnp.sum(weight * (gain - fresh) ** 2, axis=0, keepdims=True)
        norm0[1:2, :] = scale * jnp.sum(weight * (fresh - first) ** 2, axis=0, keepdims=True)
        norm0[2:3, :] = scale
        await_bytes(brecv.at[pl.ds(0, OWNERS - 1)], b_ss, b_rs, False)

    @pl.when(core == 0)
    def _():
        await_bytes(brecv, b_ss, b_rs, False)

    for f in range(2):
        for part in range(2):
            for h in range(2):
                lines = brecv[pl.ds((part * 2 + h) * 8, 8), f, :]
                at = slice(h * 8, h * 8 + 8)
                tgt[f, part, at, :] = 2.0 * swap_groups(lines) - row[f, part, at, :]

    lax.fori_loop(0, 2 * SWEEPS, sweeps, 0)

    pack(csend)
    to_owners(lambda j: csend.at[j], crecv, c_ss, c_rs)

    first_near = jnp.full((OWNERS, HALF), dest[0] // 2, jnp.int32) == near
    row_a, row_b = csend[:, 0, :], csend[:, 1, :]
    near_rows = jnp.where(first_near, row_a, row_b)
    far_rows = jnp.where(first_near, row_b, row_a)
    near_s[pl.ds(0, OWNERS), 0, :] = near_rows
    far_s[...] = far_rows.reshape(OWNERS, 1, HALF)
    slots = [jnp.full((1, HALF), dest[f] % 2, jnp.int32).astype(f32) for f in range(2)]
    near_s[pl.ds(OWNERS, 1), 0, :] = jnp.where(first_near[:1], slots[0], slots[1])
    copy_to(near_s, near_r, n_ss, n_rs, near).start()
    copy_to(far_s, far_r, f_ss, f_rs, far).start()

    @pl.when(core == 1)
    def _():
        crecv[me] = csend[chip]
        gain0 = both(arecv)
        fresh0 = both(bsend)
        weight = both(wrecv)
        scale = norm0[2:3, :]
        await_bytes(crecv.at[pl.ds(0, BANDS - 1)], c_ss, c_rs, False)
        gain = both(crecv)
        moved = gain + (gain0 - fresh0)
        coef = dot(proj[...], moved, ((1,), (0,)))
        fresh = dot(spread[...], moved, ((1,), (0,)))
        primal = scale * jnp.sum(weight * (gain - fresh) ** 2, axis=0, keepdims=True)
        dual = scale * jnp.sum(weight * (fresh - fresh0) ** 2, axis=0, keepdims=True)
        lane = iota((1, HALF), 1)
        line = jnp.zeros((1, HALF), f32)
        for n, v in enumerate((norm0[0:1, :], norm0[1:2, :], primal, dual)):
            line = jnp.where(lane == n, jnp.sum(v, axis=1, keepdims=True), line)
        esend[...] = line
        for t in range(1, DIRS):
            along(t).start()
        for k in range(4):
            dsend[k] = coef[2 * k : 2 * k + 2, :]
        dsend[4] = coef[8:10, :]
        to_plane(lambda i: dsend, drecv, d_ss, d_rs)
        drecv[chip] = dsend[...]
        for t in range(1, DIRS):
            along(t).wait_recv()
        for t in range(1, DIRS):
            line = line + erecv[t - 1]
        nsend[...] = line
        to_plane(lambda i: nsend, nrecv, m_ss, m_rs)
        nrecv[chip] = line

    await_bytes(near_r, n_ss, n_rs, False)
    await_bytes(far_r, f_ss, f_rs, False)
    slot = near_r[OWNERS, 0:1, :]
    for part in range(2):
        for h in range(2):
            at = pl.ds((part * 2 + h) * 8, 8)
            a, b = near_r[at, 0, :], far_r[at, 0, :]
            swap = jnp.broadcast_to(slot, (8, HALF)) > 0.5
            lanes = pl.ds(h * HALF, HALF)
            dlv_out[0, :, part, lanes] = jnp.where(swap, b, a)
            dlv_out[1, :, part, lanes] = jnp.where(swap, a, b)

    @pl.when(core == 1)
    def _():
        await_bytes(drecv.at[pl.ds(0, OWNERS - 1)], d_ss, d_rs, False)

    @pl.when(core == 0)
    def _():
        await_bytes(drecv, d_ss, d_rs, False)

    for c in range(TERMS):
        for part in range(2):
            for h in range(2):
                at = pl.ds((part * 2 + h) * 8, 8)
                coef_out[c, :, part, pl.ds(h * HALF, HALF)] = drecv[at, c // 2, c % 2, :]
    @pl.when(core == 1)
    def _():
        await_bytes(nrecv.at[pl.ds(0, OWNERS - 1)], m_ss, m_rs, False)

    @pl.when(core == 0)
    def _():
        await_bytes(nrecv, m_ss, m_rs, False)

    norm = jnp.sqrt(jnp.sum(nrecv[...], axis=0))
    norm_out[...] = jnp.concatenate([norm[:, 0:2], norm[:, 2:4]], axis=0)

    await_bytes(near_s, n_ss, n_rs, True)
    await_bytes(far_s, f_ss, f_rs, True)

    @pl.when(core == 1)
    def _():
        await_bytes(wrecv.at[pl.ds(0, OWNERS - 1)], w_ss, w_rs, True)
        await_bytes(asend.at[pl.ds(0, OWNERS - 1)], a_ss, a_rs, True)
        await_bytes(csend.at[pl.ds(0, OWNERS - 1)], c_ss, c_rs, True)
        await_bytes(bsend.at[pl.ds(0, BANDS - 1)], b_ss, b_rs, True)
        await_bytes(dummy, d_ss, d_rs, True)
        await_bytes(dummy.at[:, 0, pl.ds(0, 1), :], m_ss, m_rs, True)
        await_bytes(erecv, e_ss, e_rs.at[0], True)

    @pl.when(core == 0)
    def _():
        await_bytes(wrecv.at[pl.ds(0, OWNERS)], w_ss, w_rs, True)
        await_bytes(asend, a_ss, a_rs, True)
        await_bytes(csend, c_ss, c_rs, True)


def settle(*refs):
    for i in range(3):
        refs[3 + i][...] = refs[i][...]


def per_device(visibilities, sky_model, rfi_flags, destination):
    vmem = pltpu.VMEM
    dma = pltpu.SemaphoreType.DMA
    big = vmem((2, ROWS, 256, HALF), f32)
    tile = vmem((2, 256, HALF), f32)
    lines = vmem((OWNERS, 2, HALF), f32)
    every = vmem((BANDS, 2, HALF), f32)
    scratch = [
        pltpu.SMEM((2, 8, 8), jnp.int32), pltpu.SMEM((2,), jnp.int32),
        vmem((2, 8, 2, 256, 256), bf16), vmem((2, 8, 2, 256, 256), bf16),
        big, big, big, tile, tile, tile, tile,
        vmem((2, 3, ROWS, HALF), f32), vmem((2, 2, ROWS, HALF), f32),
        vmem((2, 2, ROWS, HALF), f32), vmem((2, 8, HALF), f32),
        vmem((2, HALF), f32), every, lines, every, every, lines, lines, every,
        vmem((OWNERS + 1, 1, HALF), f32), vmem((OWNERS, 1, HALF), f32),
        vmem((OWNERS + 1, 1, HALF), f32), vmem((OWNERS, 1, HALF), f32),
        vmem((5, 2, HALF), f32), vmem((OWNERS, 5, 2, HALF), f32),
        vmem((1, HALF), f32), vmem((DIRS - 1, 1, HALF), f32),
        vmem((1, HALF), f32), vmem((OWNERS, 1, HALF), f32),
        vmem((ROWS, HALF), f32), vmem((HALF, HALF), f32), vmem((8, HALF), f32),
        vmem((BANDS - 1, 5, 2, HALF), f32),
        dma((2, 8)), dma((2,)), *([dma(())] * 17), dma((DIRS - 1,)),
    ]
    hbm = pl.BlockSpec(memory_space=pl.ANY)
    inside = pl.BlockSpec(memory_space=pltpu.VMEM)
    results = pl.pallas_call(
        kernel,
        out_shape=(
            jax.ShapeDtypeStruct((2, 8, 2, 256), f32),
            jax.ShapeDtypeStruct((TERMS, 8, 2, 256), f32),
            jax.ShapeDtypeStruct((2, 2), f32),
        ),
        in_specs=[hbm] * 4,
        out_specs=(inside, inside, inside),
        scratch_shapes=scratch,
        compiler_params=pltpu.CompilerParams(
            collective_id=0, has_side_effects=True, vmem_limit_bytes=62 * 1024 * 1024
        ),
        name="admm",
    )(rfi_flags, destination, visibilities, sky_model)
    return pl.pallas_call(
        settle,
        out_shape=tuple(jax.ShapeDtypeStruct(r.shape, r.dtype) for r in results),
        name="settle",
    )(*results)


def solution(mesh):
    return jax.shard_map(
        per_device,
        mesh=mesh,
        in_specs=(
            P("band", "dir", None, None, None),
            P("band", "dir", None, None, None),
            P("band", None, None),
            P("band"),
        ),
        out_specs=(P("band", "dir", None, None), P(None, "dir", None, None), P()),
        check_vma=False,
    )
```

```python
import jax
import jax.numpy as jnp
from jax import lax
from jax.experimental import pallas as pl
from jax.experimental.pallas import tpu as pltpu
from jax.sharding import PartitionSpec as P

DEGREE = 8
SWEEPS = 4
TERMS = DEGREE + 1
BANDS = 64
OWNERS = 32
DIRS = 4
ROWS = 16
HALF = 128

f32 = jnp.float32
bf16 = jnp.bfloat16
HIGHEST = lax.Precision.HIGHEST
MESH = pl.DeviceIdType.MESH
penalty_share = 0.4


def iota(shape, dim):
    return lax.broadcasted_iota(jnp.int32, shape, dim)


def gather(x, index, axis):
    return jnp.take_along_axis(x, index, axis=axis, mode="promise_in_bounds")


def dot(a, b, contract):
    return lax.dot_general(
        a, b, (contract, ((), ())), precision=HIGHEST, preferred_element_type=f32
    )


def hops(t):
    x, z = t // 8, t % 8
    return min(x, 4 - x) + min(z, 8 - z)


FAR_FIRST = sorted(range(1, OWNERS), key=lambda t: -hops(t))
SERVED = sorted(
    ((dx, dz) for dx in range(4) for dz in range(-2, 2) if (dx, dz) != (0, 0)),
    key=lambda d: -(min(d[0], 4 - d[0]) + abs(d[1])),
)


def kernel(
    flags_hbm, dest_hbm, vis, sky, dlv_out, coef_out, norm_out,
    flags, dest, visb, skyb, are, aim, bsq, tc, tm, tp, tmag, num, row, tgt, pens,
    wsend, wrecv, asend, arecv, bsend, brecv, csend, crecv, near_s, far_s, near_r, far_r,
    dsend, drecv, esend, erecv, nsend, nrecv, proj, spread, norm0, dummy,
    in_sem, s_sem, w_ss, w_rs, a_ss, a_rs, b_ss, b_rs, c_ss, c_rs, n_ss, n_rs, f_ss, f_rs,
    d_ss, d_rs, e_ss, m_ss, m_rs, e_rs,
):
    me = lax.axis_index("band")
    plane = lax.axis_index("dir")
    chip = me // 2
    core = me - 2 * chip

    def wrapped(i, count):
        return jnp.where(i >= count, i - count, i)

    x, z = chip // 8, chip % 8
    columns = 2 * (4 * x + wrapped(z, 4))

    def copy_to(src, dst, ss, rs, target):
        return pltpu.make_async_remote_copy(
            src_ref=src, dst_ref=dst, send_sem=ss, recv_sem=rs,
            device_id={"band": target}, device_id_type=MESH,
        )

    def chunk(i, arr, buf, s):
        f, c = i // 4, lax.rem(i, 4)
        rows = pl.ds(pl.multiple_of(c * 64, 64), 64)
        return pltpu.make_async_copy(
            arr.at[f, :, :, rows, :], buf.at[f, :, :, rows, :], in_sem.at[s, i]
        )

    for i in range(8):
        chunk(i, vis, visb, 0).start()
        chunk(i, sky, skyb, 1).start()

    small = [
        pltpu.make_async_copy(flags_hbm, flags, s_sem.at[0]),
        pltpu.make_async_copy(dest_hbm, dest, s_sem.at[1]),
    ]
    for c in small:
        c.start()

    barrier = pltpu.get_barrier_semaphore()
    far = wrapped(me + BANDS // 2, BANDS)

    def greet(where):
        pl.semaphore_signal(barrier, inc=1, device_id=where, device_id_type=MESH)

    for t in FAR_FIRST:
        greet({"band": 2 * wrapped(chip + t, OWNERS) + 1})

    @pl.when(core == 0)
    def _():
        greet({"band": me + 1})
        greet({"band": far})

    @pl.when(core == 1)
    def _():
        for t in FAR_FIRST:
            greet({"band": 2 * wrapped(chip + t, OWNERS)})
        greet({"band": me - 1})
        for t in range(1, DIRS):
            greet({"dir": wrapped(plane + t, DIRS)})

    for c in small:
        c.wait()
    for f in range(2):
        count = jnp.int32(0)
        for a in range(8):
            for b in range(8):
                count = count + (1 - flags[f, a, b])
        weight = (1.0 + jnp.full((8, HALF), count, jnp.int32).astype(f32)) / 65.0
        pens[f] = penalty_share * 256.0 * weight
        wsend[pl.ds(f, 1), :] = weight[0:1, :]

    lane16 = iota((8, HALF), 1) % 16
    group = iota((8, HALF), 1) // 16
    sub = iota((8, HALF), 0)
    spread_index = [group * 16 + half * 8 + sub for half in range(2)]
    mix1 = (group + sub) % 8 * 16 + lane16
    mix2 = (sub - group + 8) % 8
    mix3 = (sub - group + 8) % 8 * 16 + lane16

    def swap_groups(x):
        return gather(gather(gather(x, mix1, 1), mix2, 0), mix3, 1)

    q_lane = iota((ROWS, HALF), 1)
    p_sub = iota((ROWS, HALF), 0)

    def operator_block(t, _):
        f, block = t // 8, t % 8

        @pl.when(block % 2 == 0)
        def _():
            chunk(t // 2, vis, visb, 0).wait()
            chunk(t // 2, sky, skyb, 1).wait()

        for qh in range(2):
            keep = [
                jnp.full((ROWS, HALF), 1 - flags[f, block, qh * 4 + b], jnp.int32)
                for b in range(4)
            ]
            kept = keep[3]
            for b in (2, 1, 0):
                kept = jnp.where(q_lane < (b + 1) * 32, keep[b], kept)
            lanes = pl.ds(qh * HALF, HALF)
            for u in range(2):
                ph = block * 2 + u
                rows = pl.ds(pl.multiple_of(ph * ROWS, ROWS), ROWS)
                apart = q_lane + qh * HALF != p_sub + ph * ROWS
                mask = jnp.where(apart, kept, 0).astype(f32).astype(bf16)[None]

                def flipped(x):
                    return x.reshape(HALF, HALF).T.astype(f32)

                mr = flipped(skyb[f, :, 0, rows, lanes] * mask)
                mi = flipped(skyb[f, :, 1, rows, lanes] * mask)
                dr = flipped(visb[f, :, 0, rows, lanes])
                di = flipped(visb[f, :, 1, rows, lanes])
                ar = mr * dr + mi * di
                ai = mr * di - mi * dr
                b2 = mr * mr + mi * mi
                are[f, ph, lanes, :] = ar
                aim[f, ph, lanes, :] = ai
                bsq[f, ph, lanes, :] = b2
                for n, v in enumerate((ar, ai, b2)):
                    part = jnp.sum(v, axis=0, keepdims=True)
                    if qh == 0:
                        num[f, n, pl.ds(ph, 1), :] = part
                    else:
                        num[f, n, pl.ds(ph, 1), :] = num[f, n, pl.ds(ph, 1), :] + part
        return 0

    lax.fori_loop(0, ROWS, operator_block, 0)

    def to_owners(src, dst, ss, rs, shared=False):
        def part(c):
            if shared:
                return src
            return src.at[pl.ds(2 * (4 * (c // 8) + wrapped(c % 8, 4)), 2)]

        for t in FAR_FIRST:
            c = wrapped(chip + t, OWNERS)
            copy_to(part(c), dst.at[me], ss, rs, 2 * c + 1).start()

        @pl.when(core == 0)
        def _():
            copy_to(part(chip), dst.at[me], ss, rs, me + 1).start()

    def to_served(src_of, dst, ss, rs):
        for dx, dz in SERVED:
            i = 2 * (8 * wrapped(x + dx, 4) + wrapped(z + dz % 8, 8))
            for k in range(2):
                copy_to(src_of(i + k), dst, ss, rs, i + k).start()
        copy_to(src_of(me - 1), dst, ss, rs, me - 1).start()

    ones = jnp.ones((ROWS, HALF), f32)
    zeros = jnp.zeros((ROWS, HALF), f32)
    for f in range(2):
        row[f, 0] = ones
        row[f, 1] = zeros
        tgt[f, 0] = ones
        tgt[f, 1] = zeros

    def update(f, odd):
        pen = jnp.concatenate([pens[f], pens[f]], axis=0)
        below = num[f, 2] + pen
        for part in range(2):
            fresh = (num[f, part] + pen * tgt[f, part]) / below
            row[f, part] = jnp.where(odd, 0.5 * (fresh + row[f, part]), fresh)

    def tile_row(f, r):
        for half in range(2):
            at = pl.ds(pl.multiple_of(r * ROWS + half * 8, 8), 8)
            c, d = [
                gather(
                    jnp.broadcast_to(row[f, part, pl.ds(r, 1), :], (8, HALF)),
                    spread_index[half],
                    1,
                )
                for part in range(2)
            ]
            tc[f, at, :] = c
            tm[f, at, :] = d - c
            tp[f, at, :] = d + c
            tmag[f, at, :] = c * c + d * d

    GROUP = 8

    def sweep(f, odd):
        def block(pb, _):
            acc = [[jnp.zeros((8, HALF), f32) for _ in range(4)] for _ in range(GROUP)]
            for q in range(32):
                at = pl.ds(q * 8, 8)
                c, m, p, g = tc[f, at, :], tm[f, at, :], tp[f, at, :], tmag[f, at, :]
                for j in range(GROUP):
                    ph = pb * GROUP + j
                    a, b = are[f, ph, at, :], aim[f, ph, at, :]
                    terms = ((a + b) * c, a * m, b * p, bsq[f, ph, at, :] * g)
                    acc[j] = [x + y for x, y in zip(acc[j], terms)]
            for j in range(GROUP):
                k1, k2, k3, below = acc[j]
                for n, v in enumerate((k1 - k3, k1 + k2, below)):
                    num[f, n, pl.ds(pb * GROUP + j, 1), :] = jnp.sum(v, axis=0, keepdims=True)
            for j in range(GROUP):
                tile_row(1 - f, pb * GROUP + j)
            return 0

        lax.fori_loop(0, ROWS // GROUP, block, 0)
        update(f, odd)

    for f in range(2):
        update(f, False)
    lax.fori_loop(0, ROWS, lambda r, _: (tile_row(0, r), 0)[1], 0, unroll=True)

    def sweeps(t, _):
        sweep(t % 2, t // 2 % 2 == 1)
        return 0

    lax.fori_loop(2, 4, sweeps, 0)

    pl.semaphore_wait(barrier, jnp.where(core == 1, BANDS - 1 + DIRS - 1, OWNERS + 1))
    to_owners(wsend, wrecv, w_ss, w_rs, shared=True)

    lax.fori_loop(4, 2 * SWEEPS, sweeps, 0)

    def natural(f):
        return [
            [swap_groups(row[f, part, h * 8 : h * 8 + 8, :]) for h in range(2)]
            for part in range(2)
        ]

    def pack(dst):
        for f in range(2):
            n = natural(f)
            for part in range(2):
                for h in range(2):
                    dst[pl.ds((part * 2 + h) * 8, 8), f, :] = n[part][h]

    pack(asend)
    to_owners(asend, arecv, a_ss, a_rs)

    def folded(v):
        v = jnp.sum(v, axis=0, keepdims=True)
        return v[:, :HALF] + v[:, HALF:]

    def along(t):
        return pltpu.make_async_remote_copy(
            src_ref=esend, dst_ref=erecv.at[t - 1], send_sem=e_ss, recv_sem=e_rs.at[t - 1],
            device_id={"dir": wrapped(plane + t, DIRS)}, device_id_type=MESH,
        )

    def both(ref):
        return jnp.concatenate([ref[:, 0, :], ref[:, 1, :]], axis=0)

    mine = pl.ds(columns, 2)

    def chunks(ref):
        return jnp.concatenate([both(ref.at[:, k]) for k in range(2)], axis=1)

    near = wrapped(me + 1, BANDS)

    def await_bytes(ref, ss, rs, sent):
        c = copy_to(ref, ref, ss, rs, near)
        c.wait_send() if sent else c.wait_recv()

    @pl.when(core == 1)
    def _():
        arecv[me] = asend[mine]
        wrecv[me] = wsend[...]
        await_bytes(wrecv.at[pl.ds(0, BANDS - 1)], w_ss, w_rs, False)
        weight = both(wrecv)
        wide = jnp.concatenate([weight, weight], axis=1)
        r = iota((HALF, HALF), 0)
        lane = iota((HALF, HALF), 1)
        band_row = (r % BANDS * 2 + r // BANDS).astype(f32)
        u = (2.0 * band_row + 1.0) / 128.0 - 1.0
        basis = jnp.where(lane == 0, 1.0, jnp.where(lane == 1, u, 0.0))
        before, now = jnp.ones_like(u), u
        for c in range(2, TERMS):
            before, now = now, 2.0 * u * now - before
            basis = jnp.where(lane == c, now, basis)
        weighted = basis * weight
        gram = dot(weighted, basis, ((0,), (0,)))[:ROWS, :]
        r16, l16 = iota((ROWS, HALF), 0), iota((ROWS, HALF), 1)
        m = jnp.where((r16 >= TERMS) & (l16 == r16), 1.0, gram)
        m = jnp.where(l16 == r16 + 16, 1.0, m)
        for c in range(TERMS):
            line = m[c : c + 1, :] / m[c : c + 1, c : c + 1]
            m = jnp.where(r16 == c, line, m - m[:, c : c + 1] * line)
        inverse = m[:, 16:32]
        proj[...] = dot(inverse, weighted[:, :ROWS], ((1,), (1,)))
        spread[...] = dot(basis[:, :ROWS], proj[...], ((1,), (0,)))
        scale = 1.0 / (16384.0 * jnp.sum(weight, axis=0, keepdims=True))

        await_bytes(arecv.at[pl.ds(0, BANDS - 1)], a_ss, a_rs, False)
        gain = chunks(arecv)
        fresh = dot(spread[...], gain, ((1,), (0,)))
        for k in range(2):
            lanes = slice(k * HALF, (k + 1) * HALF)
            for f in range(2):
                bsend[:, k, f, :] = fresh[f * BANDS : (f + 1) * BANDS, lanes]
        to_served(lambda i: bsend.at[i], brecv.at[mine], b_ss, b_rs)
        brecv[mine] = bsend[me]
        first = jnp.where(x < 2, 1.0, 0.0)
        norm0[0:1, :] = folded(wide * (gain - fresh) ** 2)
        norm0[1:2, :] = folded(wide * (fresh - first) ** 2)
        norm0[2:3, :] = scale
        await_bytes(brecv.at[pl.ds(0, OWNERS - 2)], b_ss, b_rs, False)

    @pl.when(core == 0)
    def _():
        await_bytes(brecv, b_ss, b_rs, False)

    for f in range(2):
        for part in range(2):
            for h in range(2):
                lines = brecv[pl.ds((part * 2 + h) * 8, 8), f, :]
                at = slice(h * 8, h * 8 + 8)
                tgt[f, part, at, :] = 2.0 * swap_groups(lines) - row[f, part, at, :]

    lax.fori_loop(0, 2 * SWEEPS, sweeps, 0)

    pack(csend)
    to_owners(csend, crecv, c_ss, c_rs)

    first_near = jnp.full((OWNERS, HALF), dest[0] // 2, jnp.int32) == near
    row_a, row_b = csend[:, 0, :], csend[:, 1, :]
    near_rows = jnp.where(first_near, row_a, row_b)
    far_rows = jnp.where(first_near, row_b, row_a)
    near_s[pl.ds(0, OWNERS), 0, :] = near_rows
    far_s[...] = far_rows.reshape(OWNERS, 1, HALF)
    slots = [jnp.full((1, HALF), dest[f] % 2, jnp.int32).astype(f32) for f in range(2)]
    near_s[pl.ds(OWNERS, 1), 0, :] = jnp.where(first_near[:1], slots[0], slots[1])
    copy_to(near_s, near_r, n_ss, n_rs, near).start()
    copy_to(far_s, far_r, f_ss, f_rs, far).start()

    @pl.when(core == 1)
    def _():
        crecv[me] = csend[mine]
        gain0 = chunks(arecv)
        fresh0 = chunks(bsend)
        weight = both(wrecv)
        wide = jnp.concatenate([weight, weight], axis=1)
        scale = norm0[2:3, :]
        await_bytes(crecv.at[pl.ds(0, BANDS - 1)], c_ss, c_rs, False)
        gain = chunks(crecv)
        moved = gain + (gain0 - fresh0)
        coef = dot(proj[...], moved, ((1,), (0,)))
        fresh = dot(spread[...], moved, ((1,), (0,)))
        primal = folded(wide * (gain - fresh) ** 2)
        dual = folded(wide * (fresh - fresh0) ** 2)
        lane = iota((1, HALF), 1)
        line = jnp.zeros((1, HALF), f32)
        for n, v in enumerate((norm0[0:1, :], norm0[1:2, :], primal, dual)):
            line = jnp.where(lane == n, jnp.sum(scale * v, axis=1, keepdims=True), line)
        esend[...] = line
        for t in range(1, DIRS):
            along(t).start()
        for k in range(2):
            lanes = slice(k * HALF, (k + 1) * HALF)
            for n in range(5):
                dsend[k, n] = coef[2 * n : 2 * n + 2, lanes]
        to_served(lambda i: dsend, drecv.at[mine], d_ss, d_rs)
        drecv[mine] = dsend[...]
        for t in range(1, DIRS):
            along(t).wait_recv()
        for t in range(1, DIRS):
            line = line + erecv[t - 1]
        nsend[...] = line
        group = columns // 2
        to_served(lambda i: nsend, nrecv.at[group], m_ss, m_rs)
        nrecv[group] = line

    await_bytes(near_r, n_ss, n_rs, False)
    await_bytes(far_r, f_ss, f_rs, False)
    slot = near_r[OWNERS, 0:1, :]
    for part in range(2):
        for h in range(2):
            at = pl.ds((part * 2 + h) * 8, 8)
            a, b = near_r[at, 0, :], far_r[at, 0, :]
            swap = jnp.broadcast_to(slot, (8, HALF)) > 0.5
            lanes = pl.ds(h * HALF, HALF)
            dlv_out[0, :, part, lanes] = jnp.where(swap, b, a)
            dlv_out[1, :, part, lanes] = jnp.where(swap, a, b)

    @pl.when(core == 1)
    def _():
        await_bytes(drecv.at[pl.ds(0, OWNERS - 2)], d_ss, d_rs, False)

    @pl.when(core == 0)
    def _():
        await_bytes(drecv, d_ss, d_rs, False)

    for c in range(TERMS):
        for part in range(2):
            for h in range(2):
                at = pl.ds((part * 2 + h) * 8, 8)
                coef_out[c, :, part, pl.ds(h * HALF, HALF)] = drecv[at, c // 2, c % 2, :]
    @pl.when(core == 1)
    def _():
        await_bytes(nrecv.at[pl.ds(0, OWNERS // 2 - 1)], m_ss, m_rs, False)

    @pl.when(core == 0)
    def _():
        await_bytes(nrecv, m_ss, m_rs, False)

    norm = jnp.sqrt(jnp.sum(nrecv[...], axis=0))
    norm_out[...] = jnp.concatenate([norm[:, 0:2], norm[:, 2:4]], axis=0)

    await_bytes(near_s, n_ss, n_rs, True)
    await_bytes(far_s, f_ss, f_rs, True)

    @pl.when(core == 1)
    def _():
        await_bytes(wrecv.at[pl.ds(0, OWNERS - 1)], w_ss, w_rs, True)
        await_bytes(arecv.at[pl.ds(0, OWNERS - 1)], a_ss, a_rs, True)
        await_bytes(crecv.at[pl.ds(0, OWNERS - 1)], c_ss, c_rs, True)
        await_bytes(bsend.at[pl.ds(0, OWNERS - 1)], b_ss, b_rs, True)
        await_bytes(dummy, d_ss, d_rs, True)
        await_bytes(dummy.at[:, 0, 0, pl.ds(0, 1), :], m_ss, m_rs, True)
        await_bytes(erecv, e_ss, e_rs.at[0], True)

    @pl.when(core == 0)
    def _():
        await_bytes(wrecv.at[pl.ds(0, OWNERS)], w_ss, w_rs, True)
        await_bytes(arecv.at[pl.ds(0, OWNERS)], a_ss, a_rs, True)
        await_bytes(crecv.at[pl.ds(0, OWNERS)], c_ss, c_rs, True)


def settle(*refs):
    for i in range(3):
        refs[3 + i][...] = refs[i][...]


def per_device(visibilities, sky_model, rfi_flags, destination):
    vmem = pltpu.VMEM
    dma = pltpu.SemaphoreType.DMA
    big = vmem((2, ROWS, 256, HALF), f32)
    tile = vmem((2, 256, HALF), f32)
    lines = vmem((OWNERS, 2, HALF), f32)
    every = vmem((BANDS, 2, HALF), f32)
    pairs = vmem((BANDS, 2, 2, HALF), f32)
    scratch = [
        pltpu.SMEM((2, 8, 8), jnp.int32), pltpu.SMEM((2,), jnp.int32),
        vmem((2, 8, 2, 256, 256), bf16), vmem((2, 8, 2, 256, 256), bf16),
        big, big, big, tile, tile, tile, tile,
        vmem((2, 3, ROWS, HALF), f32), vmem((2, 2, ROWS, HALF), f32),
        vmem((2, 2, ROWS, HALF), f32), vmem((2, 8, HALF), f32),
        vmem((2, HALF), f32), every, lines, pairs, pairs, lines, lines, pairs,
        vmem((OWNERS + 1, 1, HALF), f32), vmem((OWNERS, 1, HALF), f32),
        vmem((OWNERS + 1, 1, HALF), f32), vmem((OWNERS, 1, HALF), f32),
        vmem((2, 5, 2, HALF), f32), vmem((OWNERS, 5, 2, HALF), f32),
        vmem((1, HALF), f32), vmem((DIRS - 1, 1, HALF), f32),
        vmem((1, HALF), f32), vmem((OWNERS // 2, 1, HALF), f32),
        vmem((ROWS, HALF), f32), vmem((HALF, HALF), f32), vmem((8, HALF), f32),
        vmem((OWNERS - 1, 2, 5, 2, HALF), f32),
        dma((2, 8)), dma((2,)), *([dma(())] * 17), dma((DIRS - 1,)),
    ]
    hbm = pl.BlockSpec(memory_space=pl.ANY)
    inside = pl.BlockSpec(memory_space=pltpu.VMEM)
    results = pl.pallas_call(
        kernel,
        out_shape=(
            pltpu.VMEM((2, 8, 2, 256), f32),
            pltpu.VMEM((TERMS, 8, 2, 256), f32),
            pltpu.VMEM((2, 2), f32),
        ),
        in_specs=[hbm] * 4,
        out_specs=(inside, inside, inside),
        scratch_shapes=scratch,
        compiler_params=pltpu.CompilerParams(
            collective_id=0, has_side_effects=True, vmem_limit_bytes=62 * 1024 * 1024
        ),
        name="admm",
    )(rfi_flags, destination, visibilities, sky_model)
    return pl.pallas_call(
        settle,
        out_shape=tuple(jax.ShapeDtypeStruct(r.shape, r.dtype) for r in results),
        in_specs=[inside] * 3,
        out_specs=(inside,) * 3,
        compiler_params=pltpu.CompilerParams(vmem_limit_bytes=4 * 1024 * 1024),
        name="settle",
    )(*results)


def solution(mesh):
    return jax.shard_map(
        per_device,
        mesh=mesh,
        in_specs=(
            P("band", "dir", None, None, None),
            P("band", "dir", None, None, None),
            P("band", None, None),
            P("band"),
        ),
        out_specs=(P("band", "dir", None, None), P(None, "dir", None, None), P()),
        check_vma=False,
    )
```

```python
import jax
import jax.numpy as jnp
from jax import lax
from jax.experimental import pallas as pl
from jax.experimental.pallas import tpu as pltpu
from jax.sharding import PartitionSpec as P

DEGREE = 8
SWEEPS = 4
TERMS = DEGREE + 1
BANDS = 64
OWNERS = 32
DIRS = 4
ROWS = 16
HALF = 128

f32 = jnp.float32
bf16 = jnp.bfloat16
HIGHEST = lax.Precision.HIGHEST
MESH = pl.DeviceIdType.MESH
penalty_share = 0.4


def iota(shape, dim):
    return lax.broadcasted_iota(jnp.int32, shape, dim)


def gather(x, index, axis):
    return jnp.take_along_axis(x, index, axis=axis, mode="promise_in_bounds")


def dot(a, b, contract):
    return lax.dot_general(
        a, b, (contract, ((), ())), precision=HIGHEST, preferred_element_type=f32
    )


def hops(t):
    x, z = t // 8, t % 8
    return min(x, 4 - x) + min(z, 8 - z)


FAR_FIRST = sorted(range(1, OWNERS), key=lambda t: -hops(t))
SERVED = sorted(
    ((dx, dz) for dx in range(4) for dz in range(-2, 2) if (dx, dz) != (0, 0)),
    key=lambda d: -(min(d[0], 4 - d[0]) + abs(d[1])),
)


def kernel(
    flags_hbm, dest_hbm, vis, sky, dlv_out, coef_out, norm_out,
    flags, dest, visb, skyb, are, aim, bsq, tc, tm, tp, tmag, num, row, tgt, pens,
    wsend, wrecv, asend, arecv, bsend, brecv, csend, crecv, near_s, far_s, near_r, far_r,
    dsend, drecv, esend, erecv, nsend, nrecv, proj, spread, norm0, dummy,
    in_sem, s_sem, w_ss, w_rs, a_ss, a_rs, b_ss, b_rs, c_ss, c_rs, n_ss, n_rs, f_ss, f_rs,
    d_ss, d_rs, e_ss, m_ss, m_rs, e_rs,
):
    me = lax.axis_index("band")
    plane = lax.axis_index("dir")
    chip = me // 2
    core = me - 2 * chip

    def wrapped(i, count):
        return jnp.where(i >= count, i - count, i)

    x, z = chip // 8, chip % 8
    columns = 2 * (4 * x + wrapped(z, 4))

    def copy_to(src, dst, ss, rs, target):
        return pltpu.make_async_remote_copy(
            src_ref=src, dst_ref=dst, send_sem=ss, recv_sem=rs,
            device_id={"band": target}, device_id_type=MESH,
        )

    def chunk(i, arr, buf, s):
        f, c = i // 4, lax.rem(i, 4)
        rows = pl.ds(pl.multiple_of(c * 64, 64), 64)
        return pltpu.make_async_copy(
            arr.at[f, :, :, rows, :], buf.at[f, :, :, rows, :], in_sem.at[s, i]
        )

    small = [
        pltpu.make_async_copy(flags_hbm, flags, s_sem.at[0]),
        pltpu.make_async_copy(dest_hbm, dest, s_sem.at[1]),
    ]
    for c in small:
        c.start()
    for i in range(8):
        chunk(i, vis, visb, 0).start()
        chunk(i, sky, skyb, 1).start()

    barrier = pltpu.get_barrier_semaphore()
    far = wrapped(me + BANDS // 2, BANDS)

    def greet(where):
        pl.semaphore_signal(barrier, inc=1, device_id=where, device_id_type=MESH)

    for t in FAR_FIRST:
        greet({"band": 2 * wrapped(chip + t, OWNERS) + 1})

    @pl.when(core == 0)
    def _():
        greet({"band": me + 1})
        greet({"band": far})

    @pl.when(core == 1)
    def _():
        for t in FAR_FIRST:
            greet({"band": 2 * wrapped(chip + t, OWNERS)})
        greet({"band": me - 1})
        for t in range(1, DIRS):
            greet({"dir": wrapped(plane + t, DIRS)})

    for c in small:
        c.wait()
    for f in range(2):
        count = jnp.int32(0)
        for a in range(8):
            for b in range(8):
                count = count + (1 - flags[f, a, b])
        weight = (1.0 + jnp.full((8, HALF), count, jnp.int32).astype(f32)) / 65.0
        pens[f] = penalty_share * 256.0 * weight
        wsend[pl.ds(f, 1), :] = weight[0:1, :]

    lane16 = iota((8, HALF), 1) % 16
    group = iota((8, HALF), 1) // 16
    sub = iota((8, HALF), 0)
    spread_index = [group * 16 + half * 8 + sub for half in range(2)]
    mix1 = (group + sub) % 8 * 16 + lane16
    mix2 = (sub - group + 8) % 8
    mix3 = (sub - group + 8) % 8 * 16 + lane16

    def swap_groups(x):
        return gather(gather(gather(x, mix1, 1), mix2, 0), mix3, 1)

    q_lane = iota((ROWS, HALF), 1)
    p_sub = iota((ROWS, HALF), 0)

    def operator_block(t, _):
        f, four = t // 4, t % 4
        chunk(t, vis, visb, 0).wait()
        chunk(t, sky, skyb, 1).wait()

        for half, qh in [(half, qh) for half in range(2) for qh in range(2)]:
            block = four * 2 + half
            keep = [
                jnp.full((ROWS, HALF), 1 - flags[f, block, qh * 4 + b], jnp.int32)
                for b in range(4)
            ]
            kept = keep[3]
            for b in (2, 1, 0):
                kept = jnp.where(q_lane < (b + 1) * 32, keep[b], kept)
            lanes = pl.ds(qh * HALF, HALF)
            for u in range(2):
                ph = block * 2 + u
                rows = pl.ds(pl.multiple_of(ph * ROWS, ROWS), ROWS)
                apart = q_lane + qh * HALF != p_sub + ph * ROWS
                mask = jnp.where(apart, kept, 0).astype(f32).astype(bf16)[None]

                def flipped(x):
                    return x.reshape(HALF, HALF).T.astype(f32)

                mr = flipped(skyb[f, :, 0, rows, lanes] * mask)
                mi = flipped(skyb[f, :, 1, rows, lanes] * mask)
                dr = flipped(visb[f, :, 0, rows, lanes])
                di = flipped(visb[f, :, 1, rows, lanes])
                ar = mr * dr + mi * di
                ai = mr * di - mi * dr
                b2 = mr * mr + mi * mi
                are[f, ph, lanes, :] = ar
                aim[f, ph, lanes, :] = ai
                bsq[f, ph, lanes, :] = b2
                for n, v in enumerate((ar, ai, b2)):
                    part = jnp.sum(v, axis=0, keepdims=True)
                    if qh == 0:
                        num[f, n, pl.ds(ph, 1), :] = part
                    else:
                        num[f, n, pl.ds(ph, 1), :] = num[f, n, pl.ds(ph, 1), :] + part
        return 0

    lax.fori_loop(0, ROWS // 2, operator_block, 0)

    def to_owners(src, dst, ss, rs, shared=False):
        def part(c):
            if shared:
                return src
            return src.at[pl.ds(2 * (4 * (c // 8) + wrapped(c % 8, 4)), 2)]

        for t in FAR_FIRST:
            c = wrapped(chip + t, OWNERS)
            copy_to(part(c), dst.at[me], ss, rs, 2 * c + 1).start()

        @pl.when(core == 0)
        def _():
            copy_to(part(chip), dst.at[me], ss, rs, me + 1).start()

    def to_served(src_of, dst, ss, rs):
        for dx, dz in SERVED:
            i = 2 * (8 * wrapped(x + dx, 4) + wrapped(z + dz % 8, 8))
            for k in range(2):
                copy_to(src_of(i + k), dst, ss, rs, i + k).start()
        copy_to(src_of(me - 1), dst, ss, rs, me - 1).start()

    ones = jnp.ones((ROWS, HALF), f32)
    zeros = jnp.zeros((ROWS, HALF), f32)
    for f in range(2):
        row[f, 0] = ones
        row[f, 1] = zeros
        tgt[f, 0] = ones
        tgt[f, 1] = zeros

    def update(f, odd):
        pen = jnp.concatenate([pens[f], pens[f]], axis=0)
        below = num[f, 2] + pen
        for part in range(2):
            fresh = (num[f, part] + pen * tgt[f, part]) / below
            row[f, part] = jnp.where(odd, 0.5 * (fresh + row[f, part]), fresh)

    def tile_row(f, r):
        for half in range(2):
            at = pl.ds(pl.multiple_of(r * ROWS + half * 8, 8), 8)
            c, d = [
                gather(
                    jnp.broadcast_to(row[f, part, pl.ds(r, 1), :], (8, HALF)),
                    spread_index[half],
                    1,
                )
                for part in range(2)
            ]
            tc[f, at, :] = c
            tm[f, at, :] = d - c
            tp[f, at, :] = d + c
            tmag[f, at, :] = c * c + d * d

    GROUP = 8

    def sweep(f, odd):
        def block(pb, _):
            acc = [[jnp.zeros((8, HALF), f32) for _ in range(4)] for _ in range(GROUP)]
            for first, q in [(first, q) for first in (0, GROUP // 2) for q in range(32)]:
                at = pl.ds(q * 8, 8)
                c, m, p, g = tc[f, at, :], tm[f, at, :], tp[f, at, :], tmag[f, at, :]
                for j in range(first, first + GROUP // 2):
                    ph = pb * GROUP + j
                    a, b = are[f, ph, at, :], aim[f, ph, at, :]
                    terms = ((a + b) * c, a * m, b * p, bsq[f, ph, at, :] * g)
                    acc[j] = [x + y for x, y in zip(acc[j], terms)]
            for j in range(GROUP):
                k1, k2, k3, below = acc[j]
                for n, v in enumerate((k1 - k3, k1 + k2, below)):
                    num[f, n, pl.ds(pb * GROUP + j, 1), :] = jnp.sum(v, axis=0, keepdims=True)
            for j in range(GROUP):
                tile_row(1 - f, pb * GROUP + j)
            return 0

        lax.fori_loop(0, ROWS // GROUP, block, 0)
        update(f, odd)

    for f in range(2):
        update(f, False)
    lax.fori_loop(0, ROWS, lambda r, _: (tile_row(0, r), 0)[1], 0, unroll=True)

    def sweeps(t, _):
        sweep(t % 2, t // 2 % 2 == 1)
        return 0

    lax.fori_loop(2, 4, sweeps, 0)

    pl.semaphore_wait(barrier, jnp.where(core == 1, BANDS - 1 + DIRS - 1, OWNERS + 1))
    to_owners(wsend, wrecv, w_ss, w_rs, shared=True)

    lax.fori_loop(4, 2 * SWEEPS, sweeps, 0)

    def natural(f):
        return [
            [swap_groups(row[f, part, h * 8 : h * 8 + 8, :]) for h in range(2)]
            for part in range(2)
        ]

    def pack(dst):
        for f in range(2):
            n = natural(f)
            for part in range(2):
                for h in range(2):
                    dst[pl.ds((part * 2 + h) * 8, 8), f, :] = n[part][h]

    pack(asend)
    to_owners(asend, arecv, a_ss, a_rs)

    def folded(v):
        v = jnp.sum(v, axis=0, keepdims=True)
        return v[:, :HALF] + v[:, HALF:]

    def along(t):
        return pltpu.make_async_remote_copy(
            src_ref=esend, dst_ref=erecv.at[t - 1], send_sem=e_ss, recv_sem=e_rs.at[t - 1],
            device_id={"dir": wrapped(plane + t, DIRS)}, device_id_type=MESH,
        )

    def both(ref):
        return jnp.concatenate([ref[:, 0, :], ref[:, 1, :]], axis=0)

    mine = pl.ds(columns, 2)

    def chunks(ref):
        return jnp.concatenate([both(ref.at[:, k]) for k in range(2)], axis=1)

    near = wrapped(me + 1, BANDS)

    def await_bytes(ref, ss, rs, sent):
        c = copy_to(ref, ref, ss, rs, near)
        c.wait_send() if sent else c.wait_recv()

    @pl.when(core == 1)
    def _():
        arecv[me] = asend[mine]
        wrecv[me] = wsend[...]
        await_bytes(wrecv.at[pl.ds(0, BANDS - 1)], w_ss, w_rs, False)
        weight = both(wrecv)
        wide = jnp.concatenate([weight, weight], axis=1)
        r = iota((HALF, HALF), 0)
        lane = iota((HALF, HALF), 1)
        band_row = (r % BANDS * 2 + r // BANDS).astype(f32)
        u = (2.0 * band_row + 1.0) / 128.0 - 1.0
        basis = jnp.where(lane == 0, 1.0, jnp.where(lane == 1, u, 0.0))
        before, now = jnp.ones_like(u), u
        for c in range(2, TERMS):
            before, now = now, 2.0 * u * now - before
            basis = jnp.where(lane == c, now, basis)
        weighted = basis * weight
        gram = dot(weighted, basis, ((0,), (0,)))[:ROWS, :]
        r16, l16 = iota((ROWS, HALF), 0), iota((ROWS, HALF), 1)
        m = jnp.where((r16 >= TERMS) & (l16 == r16), 1.0, gram)
        m = jnp.where(l16 == r16 + 16, 1.0, m)
        for c in range(TERMS):
            line = m[c : c + 1, :] / m[c : c + 1, c : c + 1]
            m = jnp.where(r16 == c, line, m - m[:, c : c + 1] * line)
        inverse = m[:, 16:32]
        proj[...] = dot(inverse, weighted[:, :ROWS], ((1,), (1,)))
        spread[...] = dot(basis[:, :ROWS], proj[...], ((1,), (0,)))
        scale = 1.0 / (16384.0 * jnp.sum(weight, axis=0, keepdims=True))

        await_bytes(arecv.at[pl.ds(0, BANDS - 1)], a_ss, a_rs, False)
        gain = chunks(arecv)
        fresh = dot(spread[...], gain, ((1,), (0,)))
        for k in range(2):
            lanes = slice(k * HALF, (k + 1) * HALF)
            for f in range(2):
                bsend[:, k, f, :] = fresh[f * BANDS : (f + 1) * BANDS, lanes]
        to_served(lambda i: bsend.at[i], brecv.at[mine], b_ss, b_rs)
        brecv[mine] = bsend[me]
        first = jnp.where(x < 2, 1.0, 0.0)
        norm0[0:1, :] = folded(wide * (gain - fresh) ** 2)
        norm0[1:2, :] = folded(wide * (fresh - first) ** 2)
        norm0[2:3, :] = scale
        await_bytes(brecv.at[pl.ds(0, OWNERS - 2)], b_ss, b_rs, False)

    @pl.when(core == 0)
    def _():
        await_bytes(brecv, b_ss, b_rs, False)

    for f in range(2):
        for part in range(2):
            for h in range(2):
                lines = brecv[pl.ds((part * 2 + h) * 8, 8), f, :]
                at = slice(h * 8, h * 8 + 8)
                tgt[f, part, at, :] = 2.0 * swap_groups(lines) - row[f, part, at, :]

    lax.fori_loop(0, 2 * SWEEPS, sweeps, 0)

    pack(csend)
    to_owners(csend, crecv, c_ss, c_rs)

    first_near = jnp.full((OWNERS, HALF), dest[0] // 2, jnp.int32) == near
    row_a, row_b = csend[:, 0, :], csend[:, 1, :]
    near_rows = jnp.where(first_near, row_a, row_b)
    far_rows = jnp.where(first_near, row_b, row_a)
    near_s[pl.ds(0, OWNERS), 0, :] = near_rows
    far_s[...] = far_rows.reshape(OWNERS, 1, HALF)
    slots = [jnp.full((1, HALF), dest[f] % 2, jnp.int32).astype(f32) for f in range(2)]
    near_s[pl.ds(OWNERS, 1), 0, :] = jnp.where(first_near[:1], slots[0], slots[1])
    copy_to(near_s, near_r, n_ss, n_rs, near).start()
    copy_to(far_s, far_r, f_ss, f_rs, far).start()

    @pl.when(core == 1)
    def _():
        crecv[me] = csend[mine]
        gain0 = chunks(arecv)
        fresh0 = chunks(bsend)
        weight = both(wrecv)
        wide = jnp.concatenate([weight, weight], axis=1)
        scale = norm0[2:3, :]
        await_bytes(crecv.at[pl.ds(0, BANDS - 1)], c_ss, c_rs, False)
        gain = chunks(crecv)
        moved = gain + (gain0 - fresh0)
        coef = dot(proj[...], moved, ((1,), (0,)))
        fresh = dot(spread[...], moved, ((1,), (0,)))
        primal = folded(wide * (gain - fresh) ** 2)
        dual = folded(wide * (fresh - fresh0) ** 2)
        lane = iota((1, HALF), 1)
        line = jnp.zeros((1, HALF), f32)
        for n, v in enumerate((norm0[0:1, :], norm0[1:2, :], primal, dual)):
            line = jnp.where(lane == n, jnp.sum(scale * v, axis=1, keepdims=True), line)
        esend[...] = line
        for t in range(1, DIRS):
            along(t).start()
        for k in range(2):
            lanes = slice(k * HALF, (k + 1) * HALF)
            for n in range(5):
                dsend[k, n] = coef[2 * n : 2 * n + 2, lanes]
        to_served(lambda i: dsend, drecv.at[mine], d_ss, d_rs)
        drecv[mine] = dsend[...]
        for t in range(1, DIRS):
            along(t).wait_recv()
        for t in range(1, DIRS):
            line = line + erecv[t - 1]
        nsend[...] = line
        group = columns // 2
        to_served(lambda i: nsend, nrecv.at[group], m_ss, m_rs)
        nrecv[group] = line

    await_bytes(near_r, n_ss, n_rs, False)
    await_bytes(far_r, f_ss, f_rs, False)
    slot = near_r[OWNERS, 0:1, :]
    for part in range(2):
        for h in range(2):
            at = pl.ds((part * 2 + h) * 8, 8)
            a, b = near_r[at, 0, :], far_r[at, 0, :]
            swap = jnp.broadcast_to(slot, (8, HALF)) > 0.5
            lanes = pl.ds(h * HALF, HALF)
            dlv_out[0, :, part, lanes] = jnp.where(swap, b, a)
            dlv_out[1, :, part, lanes] = jnp.where(swap, a, b)

    @pl.when(core == 1)
    def _():
        await_bytes(drecv.at[pl.ds(0, OWNERS - 2)], d_ss, d_rs, False)

    @pl.when(core == 0)
    def _():
        await_bytes(drecv, d_ss, d_rs, False)

    for c in range(TERMS):
        for part in range(2):
            for h in range(2):
                at = pl.ds((part * 2 + h) * 8, 8)
                coef_out[c, :, part, pl.ds(h * HALF, HALF)] = drecv[at, c // 2, c % 2, :]
    @pl.when(core == 1)
    def _():
        await_bytes(nrecv.at[pl.ds(0, OWNERS // 2 - 1)], m_ss, m_rs, False)

    @pl.when(core == 0)
    def _():
        await_bytes(nrecv, m_ss, m_rs, False)

    norm = jnp.sqrt(jnp.sum(nrecv[...], axis=0))
    norm_out[...] = jnp.concatenate([norm[:, 0:2], norm[:, 2:4]], axis=0)

    await_bytes(near_s, n_ss, n_rs, True)
    await_bytes(far_s, f_ss, f_rs, True)

    @pl.when(core == 1)
    def _():
        await_bytes(wrecv.at[pl.ds(0, OWNERS - 1)], w_ss, w_rs, True)
        await_bytes(arecv.at[pl.ds(0, OWNERS - 1)], a_ss, a_rs, True)
        await_bytes(crecv.at[pl.ds(0, OWNERS - 1)], c_ss, c_rs, True)
        await_bytes(bsend.at[pl.ds(0, OWNERS - 1)], b_ss, b_rs, True)
        await_bytes(dummy, d_ss, d_rs, True)
        await_bytes(dummy.at[:, 0, 0, pl.ds(0, 1), :], m_ss, m_rs, True)
        await_bytes(erecv, e_ss, e_rs.at[0], True)

    @pl.when(core == 0)
    def _():
        await_bytes(wrecv.at[pl.ds(0, OWNERS)], w_ss, w_rs, True)
        await_bytes(arecv.at[pl.ds(0, OWNERS)], a_ss, a_rs, True)
        await_bytes(crecv.at[pl.ds(0, OWNERS)], c_ss, c_rs, True)


def settle(*refs):
    for i in range(3):
        refs[3 + i][...] = refs[i][...]


def per_device(visibilities, sky_model, rfi_flags, destination):
    vmem = pltpu.VMEM
    dma = pltpu.SemaphoreType.DMA
    big = vmem((2, ROWS, 256, HALF), f32)
    tile = vmem((2, 256, HALF), f32)
    lines = vmem((OWNERS, 2, HALF), f32)
    every = vmem((BANDS, 2, HALF), f32)
    pairs = vmem((BANDS, 2, 2, HALF), f32)
    scratch = [
        pltpu.SMEM((2, 8, 8), jnp.int32), pltpu.SMEM((2,), jnp.int32),
        vmem((2, 8, 2, 256, 256), bf16), vmem((2, 8, 2, 256, 256), bf16),
        big, big, big, tile, tile, tile, tile,
        vmem((2, 3, ROWS, HALF), f32), vmem((2, 2, ROWS, HALF), f32),
        vmem((2, 2, ROWS, HALF), f32), vmem((2, 8, HALF), f32),
        vmem((2, HALF), f32), every, lines, pairs, pairs, lines, lines, pairs,
        vmem((OWNERS + 1, 1, HALF), f32), vmem((OWNERS, 1, HALF), f32),
        vmem((OWNERS + 1, 1, HALF), f32), vmem((OWNERS, 1, HALF), f32),
        vmem((2, 5, 2, HALF), f32), vmem((OWNERS, 5, 2, HALF), f32),
        vmem((1, HALF), f32), vmem((DIRS - 1, 1, HALF), f32),
        vmem((1, HALF), f32), vmem((OWNERS // 2, 1, HALF), f32),
        vmem((ROWS, HALF), f32), vmem((HALF, HALF), f32), vmem((8, HALF), f32),
        vmem((OWNERS - 1, 2, 5, 2, HALF), f32),
        dma((2, 8)), dma((2,)), *([dma(())] * 17), dma((DIRS - 1,)),
    ]
    hbm = pl.BlockSpec(memory_space=pl.ANY)
    inside = pl.BlockSpec(memory_space=pltpu.VMEM)
    results = pl.pallas_call(
        kernel,
        out_shape=(
            pltpu.VMEM((2, 8, 2, 256), f32),
            pltpu.VMEM((TERMS, 8, 2, 256), f32),
            pltpu.VMEM((2, 2), f32),
        ),
        in_specs=[hbm] * 4,
        out_specs=(inside, inside, inside),
        scratch_shapes=scratch,
        compiler_params=pltpu.CompilerParams(
            collective_id=0, has_side_effects=True, vmem_limit_bytes=62 * 1024 * 1024
        ),
        name="admm",
    )(rfi_flags, destination, visibilities, sky_model)
    return pl.pallas_call(
        settle,
        out_shape=tuple(jax.ShapeDtypeStruct(r.shape, r.dtype) for r in results),
        in_specs=[inside] * 3,
        out_specs=(inside,) * 3,
        compiler_params=pltpu.CompilerParams(vmem_limit_bytes=4 * 1024 * 1024),
        name="settle",
    )(*results)


def solution(mesh):
    return jax.shard_map(
        per_device,
        mesh=mesh,
        in_specs=(
            P("band", "dir", None, None, None),
            P("band", "dir", None, None, None),
            P("band", None, None),
            P("band"),
        ),
        out_specs=(P("band", "dir", None, None), P(None, "dir", None, None), P()),
        check_vma=False,
    )
```

```python
import jax
import jax.numpy as jnp
from jax import lax
from jax.experimental import pallas as pl
from jax.experimental.pallas import tpu as pltpu
from jax.sharding import PartitionSpec as P

DEGREE = 8
SWEEPS = 4
TERMS = DEGREE + 1
BANDS = 64
OWNERS = 32
DIRS = 4
ROWS = 16
HALF = 128

f32 = jnp.float32
bf16 = jnp.bfloat16
HIGHEST = lax.Precision.HIGHEST
MESH = pl.DeviceIdType.MESH
penalty_share = 0.4


def iota(shape, dim):
    return lax.broadcasted_iota(jnp.int32, shape, dim)


def gather(x, index, axis):
    return jnp.take_along_axis(x, index, axis=axis, mode="promise_in_bounds")


def dot(a, b, contract):
    return lax.dot_general(
        a, b, (contract, ((), ())), precision=HIGHEST, preferred_element_type=f32
    )


def hops(t):
    x, z = t // 8, t % 8
    return min(x, 4 - x) + min(z, 8 - z)


FAR_FIRST = sorted(range(1, OWNERS), key=lambda t: -hops(t))
SERVED = sorted(
    ((dx, dz) for dx in range(4) for dz in range(-2, 2) if (dx, dz) != (0, 0)),
    key=lambda d: -(min(d[0], 4 - d[0]) + abs(d[1])),
)


def kernel(
    flags_hbm, dest_hbm, vis, sky, dlv_out, coef_out, norm_out,
    flags, dest, visb, skyb, are, aim, bsq, tc, tm, tp, tmag, num, row, tgt, pens,
    wsend, wrecv, asend, arecv, bsend, brecv, csend, crecv, near_s, far_s, near_r, far_r,
    dsend, drecv, esend, erecv, nsend, nrecv, proj, spread, norm0, dummy,
    in_sem, s_sem, w_ss, w_rs, a_ss, a_rs, b_ss, b_rs, c_ss, c_rs, n_ss, n_rs, f_ss, f_rs,
    d_ss, d_rs, e_ss, m_ss, m_rs, e_rs,
):
    me = lax.axis_index("band")
    plane = lax.axis_index("dir")
    chip = me // 2
    core = me - 2 * chip

    def wrapped(i, count):
        return jnp.where(i >= count, i - count, i)

    x, z = chip // 8, chip % 8
    columns = 2 * (4 * x + wrapped(z, 4))

    def copy_to(src, dst, ss, rs, target):
        return pltpu.make_async_remote_copy(
            src_ref=src, dst_ref=dst, send_sem=ss, recv_sem=rs,
            device_id={"band": target}, device_id_type=MESH,
        )

    def chunk(i, arr, buf, s):
        f, c = i // 4, lax.rem(i, 4)
        rows = pl.ds(pl.multiple_of(c * 64, 64), 64)
        return pltpu.make_async_copy(
            arr.at[f, :, :, rows, :], buf.at[f, :, :, rows, :], in_sem.at[s, i]
        )

    small = [
        pltpu.make_async_copy(flags_hbm, flags, s_sem.at[0]),
        pltpu.make_async_copy(dest_hbm, dest, s_sem.at[1]),
    ]
    for c in small:
        c.start()
    for i in range(8):
        chunk(i, vis, visb, 0).start()
        chunk(i, sky, skyb, 1).start()

    barrier = pltpu.get_barrier_semaphore()
    far = wrapped(me + BANDS // 2, BANDS)

    def greet(where):
        pl.semaphore_signal(barrier, inc=1, device_id=where, device_id_type=MESH)

    for t in FAR_FIRST:
        greet({"band": 2 * wrapped(chip + t, OWNERS) + 1})

    @pl.when(core == 0)
    def _():
        greet({"band": me + 1})
        greet({"band": far})

    @pl.when(core == 1)
    def _():
        for t in FAR_FIRST:
            greet({"band": 2 * wrapped(chip + t, OWNERS)})
        greet({"band": me - 1})
        for t in range(1, DIRS):
            greet({"dir": wrapped(plane + t, DIRS)})

    for c in small:
        c.wait()
    for f in range(2):
        count = jnp.int32(0)
        for a in range(8):
            for b in range(8):
                count = count + (1 - flags[f, a, b])
        weight = (1.0 + jnp.full((8, HALF), count, jnp.int32).astype(f32)) / 65.0
        pens[f] = penalty_share * 256.0 * weight
        wsend[pl.ds(f, 1), :] = weight[0:1, :]

    lane16 = iota((8, HALF), 1) % 16
    group = iota((8, HALF), 1) // 16
    sub = iota((8, HALF), 0)
    spread_index = [group * 16 + half * 8 + sub for half in range(2)]
    mix1 = (group + sub) % 8 * 16 + lane16
    mix2 = (sub - group + 8) % 8
    mix3 = (sub - group + 8) % 8 * 16 + lane16

    def swap_groups(x):
        return gather(gather(gather(x, mix1, 1), mix2, 0), mix3, 1)

    q_lane = iota((ROWS, HALF), 1)
    p_sub = iota((ROWS, HALF), 0)

    def operator_block(t, _):
        f, four = t // 4, t % 4
        chunk(t, vis, visb, 0).wait()
        chunk(t, sky, skyb, 1).wait()

        for half, qh in [(half, qh) for half in range(2) for qh in range(2)]:
            block = four * 2 + half
            keep = [
                jnp.full((ROWS, HALF), 1 - flags[f, block, qh * 4 + b], jnp.int32)
                for b in range(4)
            ]
            kept = keep[3]
            for b in (2, 1, 0):
                kept = jnp.where(q_lane < (b + 1) * 32, keep[b], kept)
            lanes = pl.ds(qh * HALF, HALF)
            for u in range(2):
                ph = block * 2 + u
                rows = pl.ds(pl.multiple_of(ph * ROWS, ROWS), ROWS)
                apart = q_lane + qh * HALF != p_sub + ph * ROWS
                mask = jnp.where(apart, kept, 0).astype(f32).astype(bf16)[None]

                def flipped(x):
                    return x.reshape(HALF, HALF).T.astype(f32)

                mr = flipped(skyb[f, :, 0, rows, lanes] * mask)
                mi = flipped(skyb[f, :, 1, rows, lanes] * mask)
                dr = flipped(visb[f, :, 0, rows, lanes])
                di = flipped(visb[f, :, 1, rows, lanes])
                ar = mr * dr + mi * di
                ai = mr * di - mi * dr
                b2 = mr * mr + mi * mi
                are[f, ph, lanes, :] = ar
                aim[f, ph, lanes, :] = ai
                bsq[f, ph, lanes, :] = b2
                for n, v in enumerate((ar, ai, b2)):
                    part = jnp.sum(v, axis=0, keepdims=True)
                    if qh == 0:
                        num[f, n, pl.ds(ph, 1), :] = part
                    else:
                        num[f, n, pl.ds(ph, 1), :] = num[f, n, pl.ds(ph, 1), :] + part
        return 0

    lax.fori_loop(0, ROWS // 2, operator_block, 0)

    def to_owners(src, dst, ss, rs, shared=False):
        def part(c):
            if shared:
                return src
            return src.at[pl.ds(2 * (4 * (c // 8) + wrapped(c % 8, 4)), 2)]

        for t in FAR_FIRST:
            c = wrapped(chip + t, OWNERS)
            copy_to(part(c), dst.at[me], ss, rs, 2 * c + 1).start()

        @pl.when(core == 0)
        def _():
            copy_to(part(chip), dst.at[me], ss, rs, me + 1).start()

    def to_served(src_of, dst, ss, rs):
        for dx, dz in SERVED:
            i = 2 * (8 * wrapped(x + dx, 4) + wrapped(z + dz % 8, 8))
            for k in range(2):
                copy_to(src_of(i + k), dst, ss, rs, i + k).start()
        copy_to(src_of(me - 1), dst, ss, rs, me - 1).start()

    ones = jnp.ones((ROWS, HALF), f32)
    zeros = jnp.zeros((ROWS, HALF), f32)
    for f in range(2):
        row[f, 0] = ones
        row[f, 1] = zeros
        tgt[f, 0] = ones
        tgt[f, 1] = zeros

    def update(f, odd):
        pen = jnp.concatenate([pens[f], pens[f]], axis=0)
        below = num[f, 2] + pen
        for part in range(2):
            fresh = (num[f, part] + pen * tgt[f, part]) / below
            row[f, part] = jnp.where(odd, 0.5 * (fresh + row[f, part]), fresh)

    def tile_row(f, r):
        for half in range(2):
            at = pl.ds(pl.multiple_of(r * ROWS + half * 8, 8), 8)
            c, d = [
                gather(
                    jnp.broadcast_to(row[f, part, pl.ds(r, 1), :], (8, HALF)),
                    spread_index[half],
                    1,
                )
                for part in range(2)
            ]
            tc[f, at, :] = c
            tm[f, at, :] = d - c
            tp[f, at, :] = d + c
            tmag[f, at, :] = c * c + d * d

    GROUP = 8

    def sweep(f, odd):
        def block(pb, _):
            acc = [[jnp.zeros((8, HALF), f32) for _ in range(4)] for _ in range(GROUP)]
            for first, q in [(first, q) for first in (0, GROUP // 2) for q in range(32)]:
                at = pl.ds(q * 8, 8)
                c, m, p, g = tc[f, at, :], tm[f, at, :], tp[f, at, :], tmag[f, at, :]
                for j in range(first, first + GROUP // 2):
                    ph = pb * GROUP + j
                    a, b = are[f, ph, at, :], aim[f, ph, at, :]
                    terms = ((a + b) * c, a * m, b * p, bsq[f, ph, at, :] * g)
                    acc[j] = [x + y for x, y in zip(acc[j], terms)]
            for j in range(GROUP):
                k1, k2, k3, below = acc[j]
                for n, v in enumerate((k1 - k3, k1 + k2, below)):
                    num[f, n, pl.ds(pb * GROUP + j, 1), :] = jnp.sum(v, axis=0, keepdims=True)
            for j in range(GROUP):
                tile_row(1 - f, pb * GROUP + j)
            return 0

        lax.fori_loop(0, ROWS // GROUP, block, 0)
        update(f, odd)

    for f in range(2):
        update(f, False)
    lax.fori_loop(0, ROWS, lambda r, _: (tile_row(0, r), 0)[1], 0, unroll=True)

    def sweeps(t, _):
        sweep(t % 2, t // 2 % 2 == 1)
        return 0

    lax.fori_loop(2, 4, sweeps, 0)

    pl.semaphore_wait(barrier, jnp.where(core == 1, BANDS - 1 + DIRS - 1, OWNERS + 1))
    to_owners(wsend, wrecv, w_ss, w_rs, shared=True)

    lax.fori_loop(4, 2 * SWEEPS, sweeps, 0)

    def natural(f):
        return [
            [swap_groups(row[f, part, h * 8 : h * 8 + 8, :]) for h in range(2)]
            for part in range(2)
        ]

    def pack(dst):
        for f in range(2):
            n = natural(f)
            for part in range(2):
                for h in range(2):
                    dst[pl.ds((part * 2 + h) * 8, 8), f, :] = n[part][h]

    pack(asend)
    to_owners(asend, arecv, a_ss, a_rs)

    def folded(v):
        v = jnp.sum(v, axis=0, keepdims=True)
        return v[:, :HALF] + v[:, HALF:]

    def along(t):
        return pltpu.make_async_remote_copy(
            src_ref=esend, dst_ref=erecv.at[t - 1], send_sem=e_ss, recv_sem=e_rs.at[t - 1],
            device_id={"dir": wrapped(plane + t, DIRS)}, device_id_type=MESH,
        )

    def both(ref):
        return jnp.concatenate([ref[:, 0, :], ref[:, 1, :]], axis=0)

    mine = pl.ds(columns, 2)

    def chunks(ref):
        return jnp.concatenate([both(ref.at[:, k]) for k in range(2)], axis=1)

    near = wrapped(me + 1, BANDS)

    def await_bytes(ref, ss, rs, sent):
        c = copy_to(ref, ref, ss, rs, near)
        c.wait_send() if sent else c.wait_recv()

    @pl.when(core == 1)
    def _():
        arecv[me] = asend[mine]
        wrecv[me] = wsend[...]
        await_bytes(wrecv.at[pl.ds(0, BANDS - 1)], w_ss, w_rs, False)
        weight = both(wrecv)
        wide = jnp.concatenate([weight, weight], axis=1)
        r = iota((HALF, HALF), 0)
        lane = iota((HALF, HALF), 1)
        band_row = (r % BANDS * 2 + r // BANDS).astype(f32)
        u = (2.0 * band_row + 1.0) / 128.0 - 1.0
        basis = jnp.where(lane == 0, 1.0, jnp.where(lane == 1, u, 0.0))
        before, now = jnp.ones_like(u), u
        for c in range(2, TERMS):
            before, now = now, 2.0 * u * now - before
            basis = jnp.where(lane == c, now, basis)
        weighted = basis * weight
        gram = dot(weighted, basis, ((0,), (0,)))[:ROWS, :]
        r16, l16 = iota((ROWS, HALF), 0), iota((ROWS, HALF), 1)
        m = jnp.where((r16 >= TERMS) & (l16 == r16), 1.0, gram)
        m = jnp.where(l16 == r16 + 16, 1.0, m)
        for c in range(TERMS):
            line = m[c : c + 1, :] / m[c : c + 1, c : c + 1]
            m = jnp.where(r16 == c, line, m - m[:, c : c + 1] * line)
        inverse = m[:, 16:32]
        proj[...] = dot(inverse, weighted[:, :ROWS], ((1,), (1,)))
        spread[...] = dot(basis[:, :ROWS], proj[...], ((1,), (0,)))
        scale = 1.0 / (16384.0 * jnp.sum(weight, axis=0, keepdims=True))

        await_bytes(arecv.at[pl.ds(0, BANDS - 1)], a_ss, a_rs, False)
        gain = chunks(arecv)
        fresh = dot(spread[...], gain, ((1,), (0,)))
        for k in range(2):
            lanes = slice(k * HALF, (k + 1) * HALF)
            for f in range(2):
                bsend[:, k, f, :] = fresh[f * BANDS : (f + 1) * BANDS, lanes]
        to_served(lambda i: bsend.at[i], brecv.at[mine], b_ss, b_rs)
        brecv[mine] = bsend[me]
        first = jnp.where(x < 2, 1.0, 0.0)
        norm0[0:1, :] = folded(wide * (gain - fresh) ** 2)
        norm0[1:2, :] = folded(wide * (fresh - first) ** 2)
        norm0[2:3, :] = scale
        await_bytes(brecv.at[pl.ds(0, OWNERS - 2)], b_ss, b_rs, False)

    @pl.when(core == 0)
    def _():
        await_bytes(brecv, b_ss, b_rs, False)

    for f in range(2):
        for part in range(2):
            for h in range(2):
                lines = brecv[pl.ds((part * 2 + h) * 8, 8), f, :]
                at = slice(h * 8, h * 8 + 8)
                tgt[f, part, at, :] = 2.0 * swap_groups(lines) - row[f, part, at, :]

    lax.fori_loop(0, 2 * SWEEPS, sweeps, 0)

    pack(csend)
    to_owners(csend, crecv, c_ss, c_rs)

    first_near = jnp.full((OWNERS, HALF), dest[0] // 2, jnp.int32) == near
    row_a, row_b = csend[:, 0, :], csend[:, 1, :]
    near_rows = jnp.where(first_near, row_a, row_b)
    far_rows = jnp.where(first_near, row_b, row_a)
    near_s[pl.ds(0, OWNERS), 0, :] = near_rows
    far_s[...] = far_rows.reshape(OWNERS, 1, HALF)
    slots = [jnp.full((1, HALF), dest[f] % 2, jnp.int32).astype(f32) for f in range(2)]
    near_s[pl.ds(OWNERS, 1), 0, :] = jnp.where(first_near[:1], slots[0], slots[1])
    copy_to(near_s, near_r, n_ss, n_rs, near).start()
    copy_to(far_s, far_r, f_ss, f_rs, far).start()

    @pl.when(core == 1)
    def _():
        crecv[me] = csend[mine]
        gain0 = chunks(arecv)
        fresh0 = chunks(bsend)
        weight = both(wrecv)
        wide = jnp.concatenate([weight, weight], axis=1)
        scale = norm0[2:3, :]
        await_bytes(crecv.at[pl.ds(0, BANDS - 1)], c_ss, c_rs, False)
        gain = chunks(crecv)
        moved = gain + (gain0 - fresh0)
        fresh = dot(spread[...], moved, ((1,), (0,)))
        primal = folded(wide * (gain - fresh) ** 2)
        dual = folded(wide * (fresh - fresh0) ** 2)
        lane = iota((1, HALF), 1)
        line = jnp.zeros((1, HALF), f32)
        for n, v in enumerate((norm0[0:1, :], norm0[1:2, :], primal, dual)):
            line = jnp.where(lane == n, jnp.sum(scale * v, axis=1, keepdims=True), line)
        esend[...] = line
        for t in range(1, DIRS):
            along(t).start()
        coef = dot(proj[...], moved, ((1,), (0,)))
        for k in range(2):
            lanes = slice(k * HALF, (k + 1) * HALF)
            for n in range(5):
                dsend[k, n] = coef[2 * n : 2 * n + 2, lanes]
        to_served(lambda i: dsend, drecv.at[mine], d_ss, d_rs)
        drecv[mine] = dsend[...]
        for t in range(1, DIRS):
            along(t).wait_recv()
        for t in range(1, DIRS):
            line = line + erecv[t - 1]
        nsend[...] = line
        group = columns // 2
        to_served(lambda i: nsend, nrecv.at[group], m_ss, m_rs)
        nrecv[group] = line

    await_bytes(near_r, n_ss, n_rs, False)
    await_bytes(far_r, f_ss, f_rs, False)
    slot = near_r[OWNERS, 0:1, :]
    for part in range(2):
        for h in range(2):
            at = pl.ds((part * 2 + h) * 8, 8)
            a, b = near_r[at, 0, :], far_r[at, 0, :]
            swap = jnp.broadcast_to(slot, (8, HALF)) > 0.5
            lanes = pl.ds(h * HALF, HALF)
            dlv_out[0, :, part, lanes] = jnp.where(swap, b, a)
            dlv_out[1, :, part, lanes] = jnp.where(swap, a, b)

    @pl.when(core == 1)
    def _():
        await_bytes(drecv.at[pl.ds(0, OWNERS - 2)], d_ss, d_rs, False)

    @pl.when(core == 0)
    def _():
        await_bytes(drecv, d_ss, d_rs, False)

    for c in range(TERMS):
        for part in range(2):
            for h in range(2):
                at = pl.ds((part * 2 + h) * 8, 8)
                coef_out[c, :, part, pl.ds(h * HALF, HALF)] = drecv[at, c // 2, c % 2, :]
    @pl.when(core == 1)
    def _():
        await_bytes(nrecv.at[pl.ds(0, OWNERS // 2 - 1)], m_ss, m_rs, False)

    @pl.when(core == 0)
    def _():
        await_bytes(nrecv, m_ss, m_rs, False)

    norm = jnp.sqrt(jnp.sum(nrecv[...], axis=0))
    norm_out[...] = jnp.concatenate([norm[:, 0:2], norm[:, 2:4]], axis=0)

    await_bytes(near_s, n_ss, n_rs, True)
    await_bytes(far_s, f_ss, f_rs, True)

    @pl.when(core == 1)
    def _():
        await_bytes(wrecv.at[pl.ds(0, OWNERS - 1)], w_ss, w_rs, True)
        await_bytes(arecv.at[pl.ds(0, OWNERS - 1)], a_ss, a_rs, True)
        await_bytes(crecv.at[pl.ds(0, OWNERS - 1)], c_ss, c_rs, True)
        await_bytes(bsend.at[pl.ds(0, OWNERS - 1)], b_ss, b_rs, True)
        await_bytes(dummy, d_ss, d_rs, True)
        await_bytes(dummy.at[:, 0, 0, pl.ds(0, 1), :], m_ss, m_rs, True)
        await_bytes(erecv, e_ss, e_rs.at[0], True)

    @pl.when(core == 0)
    def _():
        await_bytes(wrecv.at[pl.ds(0, OWNERS)], w_ss, w_rs, True)
        await_bytes(arecv.at[pl.ds(0, OWNERS)], a_ss, a_rs, True)
        await_bytes(crecv.at[pl.ds(0, OWNERS)], c_ss, c_rs, True)


def settle(*refs):
    for i in range(3):
        refs[3 + i][...] = refs[i][...]


def per_device(visibilities, sky_model, rfi_flags, destination):
    vmem = pltpu.VMEM
    dma = pltpu.SemaphoreType.DMA
    big = vmem((2, ROWS, 256, HALF), f32)
    tile = vmem((2, 256, HALF), f32)
    lines = vmem((OWNERS, 2, HALF), f32)
    every = vmem((BANDS, 2, HALF), f32)
    pairs = vmem((BANDS, 2, 2, HALF), f32)
    scratch = [
        pltpu.SMEM((2, 8, 8), jnp.int32), pltpu.SMEM((2,), jnp.int32),
        vmem((2, 8, 2, 256, 256), bf16), vmem((2, 8, 2, 256, 256), bf16),
        big, big, big, tile, tile, tile, tile,
        vmem((2, 3, ROWS, HALF), f32), vmem((2, 2, ROWS, HALF), f32),
        vmem((2, 2, ROWS, HALF), f32), vmem((2, 8, HALF), f32),
        vmem((2, HALF), f32), every, lines, pairs, pairs, lines, lines, pairs,
        vmem((OWNERS + 1, 1, HALF), f32), vmem((OWNERS, 1, HALF), f32),
        vmem((OWNERS + 1, 1, HALF), f32), vmem((OWNERS, 1, HALF), f32),
        vmem((2, 5, 2, HALF), f32), vmem((OWNERS, 5, 2, HALF), f32),
        vmem((1, HALF), f32), vmem((DIRS - 1, 1, HALF), f32),
        vmem((1, HALF), f32), vmem((OWNERS // 2, 1, HALF), f32),
        vmem((ROWS, HALF), f32), vmem((HALF, HALF), f32), vmem((8, HALF), f32),
        vmem((OWNERS - 1, 2, 5, 2, HALF), f32),
        dma((2, 8)), dma((2,)), *([dma(())] * 17), dma((DIRS - 1,)),
    ]
    hbm = pl.BlockSpec(memory_space=pl.ANY)
    inside = pl.BlockSpec(memory_space=pltpu.VMEM)
    results = pl.pallas_call(
        kernel,
        out_shape=(
            pltpu.VMEM((2, 8, 2, 256), f32),
            pltpu.VMEM((TERMS, 8, 2, 256), f32),
            pltpu.VMEM((2, 2), f32),
        ),
        in_specs=[hbm] * 4,
        out_specs=(inside, inside, inside),
        scratch_shapes=scratch,
        compiler_params=pltpu.CompilerParams(
            collective_id=0, has_side_effects=True, vmem_limit_bytes=62 * 1024 * 1024
        ),
        name="admm",
    )(rfi_flags, destination, visibilities, sky_model)
    return pl.pallas_call(
        settle,
        out_shape=tuple(jax.ShapeDtypeStruct(r.shape, r.dtype) for r in results),
        in_specs=[inside] * 3,
        out_specs=(inside,) * 3,
        compiler_params=pltpu.CompilerParams(vmem_limit_bytes=4 * 1024 * 1024),
        name="settle",
    )(*results)


def solution(mesh):
    return jax.shard_map(
        per_device,
        mesh=mesh,
        in_specs=(
            P("band", "dir", None, None, None),
            P("band", "dir", None, None, None),
            P("band", None, None),
            P("band"),
        ),
        out_specs=(P("band", "dir", None, None), P(None, "dir", None, None), P()),
        check_vma=False,
    )
```
